256 devices in a mesh: band: 4 (over x_lo, core), fft: 64 (over y, z, x_hi).
Axes of the slice: x: 4 (x_hi: 2, x_lo: 2; x = x_hi * 2 + x_lo), y: 4, z: 8, core: 2. Of those that a mesh axis runs over, the one named last changes fastest.
Arguments:
- orbitals: bfloat16 [16, 2, 262144], P('band', None, 'fft'), may hold values from -6 to 6
- sphere_slot: int32 [262144], P('fft'), may hold values from 0 to 24575, as said below
- stick_column: int32 [8192], P('fft'), may hold values from 0 to 36863, as said below
- potential: float32 [192, 192, 192], P('fft'), may hold values from -3 to 3
- subspace: bfloat16 [64, 2, 262144], P('band', None, 'fft'), may hold values from -0.0234375 to 0.0234375
- previous: bfloat16 [16, 2, 262144], P('band', None, 'fft'), may hold values from -6 to 6
Outputs:
- applied: bfloat16 [16, 2, 262144], P('band', None, 'fft')
- intersection: float32 [2, 64, 16], P(None, 'fft', 'band')
The draws below stay inside these ranges and needn't reach their ends.
Inputs may be any that keep to these rules, and one draw needn't show every extreme that they name: `sphere_slot`: within each aligned block of 4096 entries the values are distinct. `stick_column`: aligned block d of 128 entries holds distinct columns x * 192 + y with d * 3 <= x < (d + 1) * 3.
All inputs are finite; a program needn't handle non-finite values.
Results may differ from the reference program's by a relative error of at most 0.012.
Values may be sent and summed in bfloat16 or wider, within the bound.
A program may use at most 64 MiB of HBM per device.

```python
import jax
import jax.numpy as jnp
from jax import lax

NG = 192
STK = 128
NPW_DEV = 4096
SUBB = 64
BANDS = 16
STICKS = 8192
NPW_TOT = 262144


def draw_sphere_slot(key, part):
    blocks = NPW_TOT // NPW_DEV
    keys = jax.random.split(jax.random.fold_in(key, 11), blocks)

    def one_block(block_key):
        return jax.random.permutation(block_key, NG * STK)[:NPW_DEV].astype(jnp.int32)
    return jax.vmap(one_block)(keys).reshape(-1).astype(jnp.int32)


def draw_stick_column(key, part):
    blocks = STICKS // STK
    slab_cells = NG // blocks * NG
    keys = jax.random.split(jax.random.fold_in(key, 23), blocks)

    def one_block(block_key, owner):
        return jax.random.permutation(block_key, slab_cells)[:STK].astype(jnp.int32) + owner * slab_cells
    owners = jnp.arange(blocks, dtype=jnp.int32)
    return jax.vmap(one_block)(keys, owners).reshape(-1).astype(jnp.int32)


def strengthened(result, rng, source, target, shards_of, factor):
    def block_of(axis_at):
        return (jnp.arange(result.shape[axis_at]) // (result.shape[axis_at] // shards_of)).reshape((-1,) + (1,) * (result.ndim - 1 - axis_at))

    first = jax.random.permutation(rng, shards_of)[block_of(target)]
    other_side = (block_of(target) + shards_of // 2) % shards_of
    return jnp.where((block_of(source) == first) | (block_of(source) == other_side), factor * result, result)


def level_of(stream_key, shape, cuts, low, high):
    factor_of, own = 1.0, jax.random.fold_in(stream_key, 6)
    for position, blocks in cuts:
        steps = jnp.exp(jax.random.uniform(jax.random.fold_in(own, position), (blocks,), jnp.float32, low / len(cuts), high / len(cuts)))
        factor_of = factor_of * jnp.repeat(steps, shape[position] // blocks).reshape([-1 if axis == position else 1 for axis in range(len(shape))])
    return factor_of


def scatter_about(own_key, extent, scale, reach, pieces=(), held_as=jnp.bfloat16):
    array = scale * jax.random.normal(own_key, extent, jnp.float32)
    if pieces:
        array = array * level_of(own_key, extent, pieces, -0.22, 0.18)
    return jnp.clip(array, -reach, reach).astype(held_as)


def bell_draw_with(rng, dims, scale, reach, cuts, heavy, kind=jnp.bfloat16):
    values = scale * jax.random.normal(rng, dims, jnp.float32)
    if cuts:
        values = values * level_of(rng, dims, cuts, -0.22, 0.18)
    return jnp.clip(strengthened(values, jax.random.fold_in(rng, 3), *heavy), -reach, reach).astype(kind)


def setup_inputs(seed: int = 0) -> dict:
    seeds = jax.random.split(jax.random.key(seed), 7)
    return {
        "orbitals": scatter_about(seeds[0], (BANDS, 2, NPW_TOT), 1.0, 6.0, ((0, 4), (2, 64))),
        "sphere_slot": draw_sphere_slot(jax.random.fold_in(seeds[6], 71), 0),
        "stick_column": draw_stick_column(jax.random.fold_in(seeds[6], 71), 0),
        "potential": jnp.clip(jax.random.uniform(seeds[3], (NG, NG, NG), jnp.float32, -3.0, 3.0) * level_of(seeds[3], (NG, NG, NG), ((0, 64),), -0.4, 0.0), -3.0, 3.0),
        "subspace": bell_draw_with(seeds[4], (SUBB, 2, NPW_TOT), (2 * NPW_TOT) ** -0.5, 0.0234375, ((0, 4), (2, 64)), (2, 0, 64, 4.0)),
        "previous": scatter_about(seeds[5], (BANDS, 2, NPW_TOT), 1.0, 6.0, ((0, 4), (2, 64))),
    }


def frequency(values, grid_size):
    return jnp.where(values >= grid_size // 2, values - grid_size, values).astype(jnp.float32)


def rounded(values):
    real_part = lax.optimization_barrier(jnp.real(values).astype(jnp.bfloat16)).astype(jnp.float32)
    imag_part = lax.optimization_barrier(jnp.imag(values).astype(jnp.bfloat16)).astype(jnp.float32)
    return lax.complex(real_part, imag_part)


def reference(orbitals, sphere_slot, stick_column, potential, subspace, previous):
    owner = jnp.arange(NPW_TOT, dtype=jnp.int32) // NPW_DEV
    plane_index = (sphere_slot // STK).astype(jnp.int32)
    column = stick_column[(owner * STK + sphere_slot % STK).astype(jnp.int32)]
    cell = (plane_index * (NG * NG) + column).astype(jnp.int32)
    freq_z = frequency(plane_index, NG)
    freq_x = frequency(column // NG, NG)
    freq_y = frequency(column % NG, NG)
    kinetic = (freq_z * freq_z + freq_x * freq_x + freq_y * freq_y) * (2.0 / (NG * NG))

    def one_band(coeffs):
        real_in = coeffs[0].astype(jnp.float32)
        imag_in = coeffs[1].astype(jnp.float32)
        empty = jnp.zeros((NG * NG * NG,), jnp.float32)
        grid = lax.complex(empty.at[cell].set(real_in), empty.at[cell].set(imag_in)).reshape(NG, NG, NG)
        grid = rounded(jnp.fft.ifft(grid, axis=0, norm="forward"))
        grid = rounded(jnp.fft.ifft(grid, axis=2, norm="forward"))
        grid = rounded(jnp.fft.ifft(grid, axis=1, norm="forward") * potential)
        grid = rounded(jnp.fft.fft(grid, axis=1, norm="forward"))
        grid = rounded(jnp.fft.fft(grid, axis=2, norm="forward"))
        grid = jnp.fft.fft(grid, axis=0, norm="forward")
        values = grid.reshape(-1)[cell]
        applied_real = jnp.real(values) + kinetic * real_in
        applied_imag = jnp.imag(values) + kinetic * imag_in
        return jnp.stack([applied_real, applied_imag]).astype(jnp.bfloat16)

    applied = lax.map(one_band, orbitals)
    sub_real = subspace[:, 0]
    sub_imag = subspace[:, 1]
    prev_real = previous[:, 0]
    prev_imag = previous[:, 1]
    over_real = jnp.dot(sub_real, prev_real.T, preferred_element_type=jnp.float32) + jnp.dot(sub_imag, prev_imag.T, preferred_element_type=jnp.float32)
    over_imag = jnp.dot(sub_real, prev_imag.T, preferred_element_type=jnp.float32) - jnp.dot(sub_imag, prev_real.T, preferred_element_type=jnp.float32)
    return applied, jnp.stack([over_real, over_imag])
```

```python
import functools
import math

import jax
import jax.numpy as jnp
import numpy as np
from jax import lax
from jax.experimental import pallas as pl
from jax.experimental.pallas import tpu as pltpu
from jax.sharding import PartitionSpec as P

F32 = jnp.float32
BF16 = jnp.bfloat16
NT = (((1,), (1,)), ((), ()))


def dot(a, b):
    return jnp.dot(a, b, preferred_element_type=F32)


def dot_nt(a, b):
    return lax.dot_general(a, b, NT, preferred_element_type=F32)


def tables(grid, owners):
    depth = grid // owners
    groups = owners // 4
    k = np.arange(grid)
    angle = 2.0 * math.pi * ((k[:, None] * k[None, :]) % grid) / grid
    cos, sin = np.cos(angle), np.sin(angle)
    icos, isin = cos / grid, -sin / grid
    zorder = np.arange(grid)
    zorder = (zorder % owners) * depth + zorder // owners
    rows = np.full(groups * 16, -1)
    for g in range(groups):
        rows[16 * g : 16 * g + 4 * depth] = 4 * depth * g + np.arange(4 * depth)

    def padded(table):
        out = np.zeros((groups * 16, grid))
        out[rows >= 0] = table[rows[rows >= 0]]
        return out

    def trio(c, s):
        return [jnp.asarray(t, BF16) for t in (c, s, -s)]

    zf = trio(cos[zorder], sin[zorder])
    zb = trio(icos[zorder], isin[zorder])
    yf = trio(cos, sin)
    yb = trio(icos, isin)
    xf = trio(padded(cos).T, padded(sin).T)
    xb = trio(padded(icos), padded(isin))
    return zf, zb, yf, yb, xf, xb


def vmem():
    return pl.BlockSpec(memory_space=pltpu.VMEM)


def call(body, outs, scratch, name):
    single = not isinstance(outs, (list, tuple))
    return pl.pallas_call(
        body,
        out_shape=outs,
        out_specs=vmem() if single else [vmem() for _ in outs],
        scratch_shapes=scratch,
        compiler_params=pltpu.CompilerParams(vmem_limit_bytes=60 * 2**20),
        name=name,
    )


def forward_z(orb, slot, zf, send, stick_hot, plane_hot, stage):
    bands = orb.shape[0] // 2
    sticks, grid = stick_hot.shape[0], plane_hot.shape[0]
    owners = send.shape[0]
    depth = grid // owners
    rows = 2 * bands * depth
    chunk = 512
    for c in range(0, slot.shape[1], chunk):
        sl = slot[:, c : c + chunk]
        stick = lax.rem(sl, sticks)
        plane = lax.div(sl, sticks)
        stick_hot[:, c : c + chunk] = (
            lax.broadcasted_iota(jnp.int32, (sticks, chunk), 0) == stick
        ).astype(F32).astype(BF16)
        plane_hot[:, c : c + chunk] = (
            lax.broadcasted_iota(jnp.int32, (grid, chunk), 0) == plane
        ).astype(F32).astype(BF16)
    zc, zs, zn = (t[...] for t in zf)
    for b in range(bands):
        parts = []
        for p in range(2):
            lhs = stick_hot[...] * orb[2 * b + p : 2 * b + p + 1, :]
            parts.append(dot_nt(lhs, plane_hot[...]).astype(BF16))
        re, im = parts
        out = (
            dot_nt(zc, re) + dot_nt(zn, im),
            dot_nt(zs, re) + dot_nt(zc, im),
        )
        for p in range(2):
            for z in range(depth):
                row = (p * bands + b) * depth + z
                stage[pl.ds(row, owners, stride=rows), :] = out[p][z * owners : (z + 1) * owners]
    for f in range(owners):
        send[f] = stage[rows * f : rows * (f + 1), :].astype(BF16)


def build_masks(cols, ymask, xmask, grid, depth):
    groups = ymask.shape[0]
    sticks = cols.shape[1]
    for g in range(groups):
        for d in range(4):
            col = cols[4 * g + d : 4 * g + d + 1, :]
            x = lax.div(col, grid)
            y = col - x * grid
            x = x - 4 * depth * g
            lanes = slice(sticks * d, sticks * (d + 1))
            ymask[g, :, lanes] = (
                lax.broadcasted_iota(jnp.int32, (grid, sticks), 0) == y
            ).astype(F32).astype(BF16)
            xmask[g, :, lanes] = (
                lax.broadcasted_iota(jnp.int32, (16, sticks), 0) == x
            ).astype(F32)


def plane_work(recv, pot, yf, yb, xf, xb, send, ymask, xmask, val, are, aim, back):
    groups = ymask.shape[0]
    rows = recv.shape[1]
    half = rows // 2
    depth = pot.shape[0]
    sticks = recv.shape[2]
    grid = pot.shape[1]
    wide = 4 * sticks

    def scatter(g, carry):
        for d in range(4):
            val[:, sticks * d : sticks * (d + 1)] = recv[4 * g + d].astype(F32)
        mask = xmask[g]
        parts = []
        for p in range(2):
            lhs = jnp.concatenate(
                [(mask * val[r : r + 1, :]).astype(BF16) for r in range(p * half, (p + 1) * half)],
                axis=0,
            )
            parts.append(dot_nt(lhs, ymask[g]).astype(BF16))
        re, im = parts
        at = pl.ds(pl.multiple_of(16 * g, 16), 16)
        are[:, at, :] = (dot(re, yf[0][...]) + dot(im, yf[2][...])).astype(BF16).reshape(half, 16, grid)
        aim[:, at, :] = (dot(re, yf[1][...]) + dot(im, yf[0][...])).astype(BF16).reshape(half, 16, grid)
        return carry

    lax.fori_loop(0, groups, scatter, 0)

    def local(r, carry):
        z = lax.rem(r, depth)
        v = pot[z]
        re, im = are[r], aim[r]
        wr = ((dot(xf[0][...], re) + dot(xf[2][...], im)) * v).astype(BF16)
        wi = ((dot(xf[1][...], re) + dot(xf[0][...], im)) * v).astype(BF16)
        br = (dot(xb[0][...], wr) + dot(xb[2][...], wi)).astype(BF16)
        bi = (dot(xb[1][...], wr) + dot(xb[0][...], wi)).astype(BF16)
        back[r] = (dot(br, yb[0][...]) + dot(bi, yb[2][...])).astype(BF16)
        back[half + r] = (dot(br, yb[1][...]) + dot(bi, yb[0][...])).astype(BF16)
        return carry

    lax.fori_loop(0, half, local, 0)

    def pick(g, carry):
        mask = xmask[g]
        at = pl.ds(pl.multiple_of(16 * g, 16), 16)
        lhs = back[:, at, :].reshape(rows * 16, grid)
        t = dot(lhs, ymask[g]).reshape(rows, 16, wide)
        got = jnp.sum(t * mask[None], axis=1)
        for d in range(4):
            send[4 * g + d] = got[:, sticks * d : sticks * (d + 1)].astype(BF16)
        return carry

    lax.fori_loop(0, groups, pick, 0)


def frequency(values, grid):
    return jnp.where(values >= grid // 2, values - grid, values).astype(F32)


def backward_z(recv, orb, slot, column, zb, out, stage, stick_hot, plane_hot):
    owners, rows, sticks = recv.shape
    bands = orb.shape[0] // 2
    grid = zb[0].shape[0]
    depth = grid // owners
    chunk = 512
    for f in range(owners):
        stage[rows * f : rows * (f + 1), :] = recv[f].astype(F32)
    col = column[...]
    x = lax.div(col, grid)
    y = col - x * grid
    coords = jnp.concatenate([x, y, x, y, x, y, x, y], axis=0).astype(F32).astype(BF16)
    lines = []
    zc, zs, zn = (t[...] for t in zb)
    for b in range(bands):
        parts = []
        for p in range(2):
            cut = []
            for z in range(depth):
                row = (p * bands + b) * depth + z
                cut.append(stage[pl.ds(row, owners, stride=rows), :])
            parts.append(jnp.concatenate(cut, axis=0).T.astype(BF16))
        re, im = parts
        lines.append((dot(re, zc) + dot(im, zn)).astype(BF16))
        lines.append((dot(re, zs) + dot(im, zc)).astype(BF16))
    for c in range(0, slot.shape[1], chunk):
        cut = slice(c, c + chunk)
        sl = slot[:, cut]
        stick = lax.rem(sl, sticks)
        plane = lax.div(sl, sticks)
        hot = lax.broadcasted_iota(jnp.int32, (sticks, chunk), 0) == stick
        phot = (lax.broadcasted_iota(jnp.int32, (grid, chunk), 0) == plane).astype(F32).astype(BF16)
        shot = hot.astype(F32)
        xy = dot(coords, shot.astype(BF16))
        fz = frequency(plane, grid)
        fx = frequency(xy[0:1].astype(jnp.int32), grid)
        fy = frequency(xy[1:2].astype(jnp.int32), grid)
        kinetic = (fz * fz + fx * fx + fy * fy) * (2.0 / (grid * grid))
        got = []
        for line in lines:
            t = dot(line, phot)
            got.append(jnp.sum(t * shot, axis=0, keepdims=True))
        out[:, cut] = (
            jnp.concatenate(got, axis=0) + kinetic * orb[:, cut].astype(F32)
        ).astype(BF16)


def kernel_one(orb, slot, zc, zs, zn, send, stick_hot, plane_hot, stage):
    forward_z(orb, slot, (zc, zs, zn), send, stick_hot, plane_hot, stage)


def kernel_two(recv, cols, pot, *rest):
    yf, yb, xf, xb = (rest[3 * i : 3 * i + 3] for i in range(4))
    send, ymask, xmask, val, are, aim, back = rest[12:]
    build_masks(cols, ymask, xmask, pot.shape[1], pot.shape[0])
    plane_work(recv, pot, yf, yb, xf, xb, send, ymask, xmask, val, are, aim, back)


def kernel_three(recv, orb, slot, column, zc, zs, zn, out, stage):
    backward_z(recv, orb, slot, column, (zc, zs, zn), out, stage, None, None)


def per_device(orbitals, sphere_slot, stick_column, potential, subspace, previous):
    owners = lax.axis_size("fft")
    groups = owners // 4
    grid = potential.shape[1]
    depth = potential.shape[0]
    sticks = stick_column.shape[0]
    waves = sphere_slot.shape[0]
    bands = orbitals.shape[0]
    rows = 2 * bands * depth
    zf, zb, yf, yb, xf, xb = tables(grid, owners)
    orb = orbitals.reshape(2 * bands, waves)
    slot = sphere_slot.reshape(1, waves)
    column = stick_column.reshape(1, sticks)

    def sds(shape, kind):
        return jax.ShapeDtypeStruct(shape, kind)

    message = sds((owners, rows, sticks), BF16)
    send = call(
        kernel_one,
        message,
        [
            pltpu.VMEM((sticks, waves), BF16),
            pltpu.VMEM((grid, waves), BF16),
            pltpu.VMEM((owners * rows, sticks), F32),
        ],
        "forward_z",
    )(orb, slot, *zf)
    cols = lax.all_gather(stick_column, "fft")
    recv = lax.all_to_all(send, "fft", 0, 0, tiled=True)
    send = call(
        kernel_two,
        message,
        [
            pltpu.VMEM((groups, grid, 4 * sticks), BF16),
            pltpu.VMEM((groups, 16, 4 * sticks), F32),
            pltpu.VMEM((rows, 4 * sticks), F32),
            pltpu.VMEM((rows // 2, groups * 16, grid), BF16),
            pltpu.VMEM((rows // 2, groups * 16, grid), BF16),
            pltpu.VMEM((rows, groups * 16, grid), BF16),
        ],
        "planes",
    )(recv, cols, potential, *yf, *yb, *xf, *xb)
    recv = lax.all_to_all(send, "fft", 0, 0, tiled=True)
    applied = call(
        kernel_three,
        sds((2 * bands, waves), BF16),
        [pltpu.VMEM((owners * rows, sticks), F32)],
        "backward_z",
    )(recv, orb, slot, column, *zb)
    applied = applied.reshape(orbitals.shape)

    every = lax.all_gather(previous, "band")
    every = every.reshape(-1, 2, waves)
    sr, si = subspace[:, 0], subspace[:, 1]
    pr, pi = every[:, 0], every[:, 1]
    own = jnp.stack([dot_nt(sr, pr) + dot_nt(si, pi), dot_nt(sr, pi) - dot_nt(si, pr)])
    groups_of = lax.axis_size("band")
    tiles = own.reshape(2, own.shape[1], groups_of, bands)
    tiles = lax.all_to_all(jnp.moveaxis(tiles, 2, 0), "band", 0, 0, tiled=True)
    tiles = jnp.moveaxis(tiles, 1, 2).reshape(-1, 2, bands)
    tiles = lax.all_to_all(tiles[:, None], "fft", 0, 1, tiled=True)
    intersection = jnp.moveaxis(jnp.sum(tiles, axis=1), 0, 1)
    return applied, intersection


def solution(mesh):
    return jax.shard_map(
        per_device,
        mesh=mesh,
        in_specs=(
            P("band", None, "fft"),
            P("fft"),
            P("fft"),
            P("fft", None, None),
            P("band", None, "fft"),
            P("band", None, "fft"),
        ),
        out_specs=(P("band", None, "fft"), P(None, "fft", "band")),
        check_vma=False,
    )
```

```python
import functools
import math

import jax
import jax.numpy as jnp
import numpy as np
from jax import lax
from jax.experimental import pallas as pl
from jax.experimental.pallas import tpu as pltpu
from jax.sharding import PartitionSpec as P

F32 = jnp.float32
BF16 = jnp.bfloat16
NT = (((1,), (1,)), ((), ()))


def dot(a, b):
    return jnp.dot(a, b, preferred_element_type=F32)


def dot_nt(a, b):
    return lax.dot_general(a, b, NT, preferred_element_type=F32)


def tables(grid, owners):
    depth = grid // owners
    groups = owners // 4
    k = np.arange(grid)
    angle = 2.0 * math.pi * ((k[:, None] * k[None, :]) % grid) / grid
    cos, sin = np.cos(angle), np.sin(angle)
    icos, isin = cos / grid, -sin / grid
    zorder = np.arange(grid)
    zorder = (zorder % owners) * depth + zorder // owners
    rows = np.full(groups * 16, -1)
    for g in range(groups):
        rows[16 * g : 16 * g + 4 * depth] = 4 * depth * g + np.arange(4 * depth)

    def padded(table):
        out = np.zeros((groups * 16, grid))
        out[rows >= 0] = table[rows[rows >= 0]]
        return out

    def trio(c, s):
        return [jnp.asarray(t, BF16) for t in (c, s, -s)]

    zf = trio(cos[zorder], sin[zorder])
    zb = trio(icos[zorder], isin[zorder])
    yf = trio(cos, sin)
    yb = trio(icos, isin)
    xf = trio(padded(cos).T, padded(sin).T)
    xb = trio(padded(icos), padded(isin))
    return zf, zb, yf, yb, xf, xb


def vmem():
    return pl.BlockSpec(memory_space=pltpu.VMEM)


def call(body, outs, scratch, name):
    single = not isinstance(outs, (list, tuple))
    return pl.pallas_call(
        body,
        out_shape=outs,
        out_specs=vmem() if single else [vmem() for _ in outs],
        scratch_shapes=scratch,
        compiler_params=pltpu.CompilerParams(vmem_limit_bytes=60 * 2**20),
        name=name,
    )


def forward_z(orb, slot, zf, send, stick_hot, plane_hot, stage):
    bands = orb.shape[0] // 2
    sticks, grid = stick_hot.shape[0], plane_hot.shape[0]
    owners = send.shape[0]
    depth = grid // owners
    rows = 2 * bands * depth
    chunk = 512
    for c in range(0, slot.shape[1], chunk):
        sl = slot[:, c : c + chunk]
        stick = lax.rem(sl, sticks)
        plane = lax.div(sl, sticks)
        stick_hot[:, c : c + chunk] = (
            lax.broadcasted_iota(jnp.int32, (sticks, chunk), 0) == stick
        ).astype(F32).astype(BF16)
        plane_hot[:, c : c + chunk] = (
            lax.broadcasted_iota(jnp.int32, (grid, chunk), 0) == plane
        ).astype(F32).astype(BF16)
    zc, zs, zn = (t[...] for t in zf)
    for b in range(bands):
        parts = []
        for p in range(2):
            lhs = stick_hot[...] * orb[2 * b + p : 2 * b + p + 1, :]
            parts.append(dot_nt(lhs, plane_hot[...]).astype(BF16))
        re, im = parts
        out = (
            dot_nt(zc, re) + dot_nt(zn, im),
            dot_nt(zs, re) + dot_nt(zc, im),
        )
        for p in range(2):
            for z in range(depth):
                row = (p * bands + b) * depth + z
                stage[pl.ds(row, owners, stride=rows), :] = out[p][z * owners : (z + 1) * owners]
    for f in range(owners):
        send[f] = stage[rows * f : rows * (f + 1), :].astype(BF16)


def build_masks(cols, ymask, xmask, grid, depth):
    groups = ymask.shape[0]
    sticks = cols.shape[1]
    for g in range(groups):
        for d in range(4):
            col = cols[4 * g + d : 4 * g + d + 1, :]
            x = lax.div(col, grid)
            y = col - x * grid
            x = x - 4 * depth * g
            lanes = slice(sticks * d, sticks * (d + 1))
            ymask[g, :, lanes] = (
                lax.broadcasted_iota(jnp.int32, (grid, sticks), 0) == y
            ).astype(F32).astype(BF16)
            xmask[g, :, lanes] = (
                lax.broadcasted_iota(jnp.int32, (16, sticks), 0) == x
            ).astype(F32)


def plane_work(recv, pot, yf, yb, xf, xb, send, ymask, xmask, val, are, aim, back):
    groups = ymask.shape[0]
    rows = recv.shape[1]
    half = rows // 2
    depth = pot.shape[0]
    sticks = recv.shape[2]
    grid = pot.shape[1]
    wide = 4 * sticks

    def scatter(g, carry):
        for d in range(4):
            val[:, sticks * d : sticks * (d + 1)] = recv[4 * g + d].astype(F32)
        mask = xmask[g]
        parts = []
        for p in range(2):
            lhs = jnp.concatenate(
                [(mask * val[r : r + 1, :]).astype(BF16) for r in range(p * half, (p + 1) * half)],
                axis=0,
            )
            parts.append(dot_nt(lhs, ymask[g]).astype(BF16))
        re, im = parts
        at = pl.ds(pl.multiple_of(16 * g, 16), 16)
        are[:, at, :] = (dot(re, yf[0][...]) + dot(im, yf[2][...])).astype(BF16).reshape(half, 16, grid)
        aim[:, at, :] = (dot(re, yf[1][...]) + dot(im, yf[0][...])).astype(BF16).reshape(half, 16, grid)
        return carry

    lax.fori_loop(0, groups, scatter, 0)

    def local(r, carry):
        z = lax.rem(r, depth)
        v = pot[z]
        re, im = are[r], aim[r]
        wr = ((dot(xf[0][...], re) + dot(xf[2][...], im)) * v).astype(BF16)
        wi = ((dot(xf[1][...], re) + dot(xf[0][...], im)) * v).astype(BF16)
        br = (dot(xb[0][...], wr) + dot(xb[2][...], wi)).astype(BF16)
        bi = (dot(xb[1][...], wr) + dot(xb[0][...], wi)).astype(BF16)
        back[r] = (dot(br, yb[0][...]) + dot(bi, yb[2][...])).astype(BF16)
        back[half + r] = (dot(br, yb[1][...]) + dot(bi, yb[0][...])).astype(BF16)
        return carry

    lax.fori_loop(0, half, local, 0)

    def pick(g, carry):
        mask = xmask[g]
        at = pl.ds(pl.multiple_of(16 * g, 16), 16)
        lhs = back[:, at, :].reshape(rows * 16, grid)
        t = dot(lhs, ymask[g]).reshape(rows, 16, wide)
        got = jnp.sum(t * mask[None], axis=1)
        for d in range(4):
            send[4 * g + d] = got[:, sticks * d : sticks * (d + 1)].astype(BF16)
        return carry

    lax.fori_loop(0, groups, pick, 0)


def frequency(values, grid):
    return jnp.where(values >= grid // 2, values - grid, values).astype(F32)


def backward_z(recv, orb, slot, column, zb, out, stage, stick_hot, plane_hot):
    owners, rows, sticks = recv.shape
    bands = orb.shape[0] // 2
    grid = zb[0].shape[0]
    depth = grid // owners
    chunk = 512
    for f in range(owners):
        stage[rows * f : rows * (f + 1), :] = recv[f].astype(F32)
    col = column[...]
    x = lax.div(col, grid)
    y = col - x * grid
    coords = jnp.concatenate([x, y, x, y, x, y, x, y], axis=0).astype(F32).astype(BF16)
    lines = []
    zc, zs, zn = (t[...] for t in zb)
    for b in range(bands):
        parts = []
        for p in range(2):
            cut = []
            for z in range(depth):
                row = (p * bands + b) * depth + z
                cut.append(stage[pl.ds(row, owners, stride=rows), :])
            parts.append(jnp.concatenate(cut, axis=0).T.astype(BF16))
        re, im = parts
        lines.append((dot(re, zc) + dot(im, zn)).astype(BF16))
        lines.append((dot(re, zs) + dot(im, zc)).astype(BF16))
    for c in range(0, slot.shape[1], chunk):
        cut = slice(c, c + chunk)
        sl = slot[:, cut]
        stick = lax.rem(sl, sticks)
        plane = lax.div(sl, sticks)
        hot = lax.broadcasted_iota(jnp.int32, (sticks, chunk), 0) == stick
        phot = (lax.broadcasted_iota(jnp.int32, (grid, chunk), 0) == plane).astype(F32).astype(BF16)
        shot = hot.astype(F32)
        xy = dot(coords, shot.astype(BF16))
        fz = frequency(plane, grid)
        fx = frequency(xy[0:1].astype(jnp.int32), grid)
        fy = frequency(xy[1:2].astype(jnp.int32), grid)
        kinetic = (fz * fz + fx * fx + fy * fy) * (2.0 / (grid * grid))
        got = []
        for line in lines:
            t = dot(line, phot)
            got.append(jnp.sum(t * shot, axis=0, keepdims=True))
        out[:, cut] = (
            jnp.concatenate(got, axis=0) + kinetic * orb[:, cut].astype(F32)
        ).astype(BF16)


def kernel_one(orb, slot, zc, zs, zn, send, stick_hot, plane_hot, stage):
    forward_z(orb, slot, (zc, zs, zn), send, stick_hot, plane_hot, stage)


def kernel_two(recv, cols, pot, *rest):
    yf, yb, xf, xb = (rest[3 * i : 3 * i + 3] for i in range(4))
    send, ymask, xmask, val, are, aim, back = rest[12:]
    build_masks(cols, ymask, xmask, pot.shape[1], pot.shape[0])
    plane_work(recv, pot, yf, yb, xf, xb, send, ymask, xmask, val, are, aim, back)


def kernel_three(recv, orb, slot, column, zc, zs, zn, out, stage):
    backward_z(recv, orb, slot, column, (zc, zs, zn), out, stage, None, None)


def per_device(orbitals, sphere_slot, stick_column, potential, subspace, previous):
    owners = lax.axis_size("fft")
    groups = owners // 4
    grid = potential.shape[1]
    depth = potential.shape[0]
    sticks = stick_column.shape[0]
    waves = sphere_slot.shape[0]
    bands = orbitals.shape[0]
    rows = 2 * bands * depth
    zf, zb, yf, yb, xf, xb = tables(grid, owners)
    orb = orbitals.reshape(2 * bands, waves)
    slot = sphere_slot.reshape(1, waves)
    column = stick_column.reshape(1, sticks)

    def sds(shape, kind):
        return jax.ShapeDtypeStruct(shape, kind)

    message = sds((owners, rows, sticks), BF16)
    send = call(
        kernel_one,
        message,
        [
            pltpu.VMEM((sticks, waves), BF16),
            pltpu.VMEM((grid, waves), BF16),
            pltpu.VMEM((owners * rows, sticks), F32),
        ],
        "forward_z",
    )(orb, slot, *zf)
    cols = jnp.broadcast_to(stick_column[None], (owners, sticks))
    cols = lax.all_to_all(cols, "fft", 0, 0, tiled=True)
    recv = lax.all_to_all(send, "fft", 0, 0, tiled=True)
    send = call(
        kernel_two,
        message,
        [
            pltpu.VMEM((groups, grid, 4 * sticks), BF16),
            pltpu.VMEM((groups, 16, 4 * sticks), F32),
            pltpu.VMEM((rows, 4 * sticks), F32),
            pltpu.VMEM((rows // 2, groups * 16, grid), BF16),
            pltpu.VMEM((rows // 2, groups * 16, grid), BF16),
            pltpu.VMEM((rows, groups * 16, grid), BF16),
        ],
        "planes",
    )(recv, cols, potential, *yf, *yb, *xf, *xb)
    recv = lax.all_to_all(send, "fft", 0, 0, tiled=True)
    applied = call(
        kernel_three,
        sds((2 * bands, waves), BF16),
        [pltpu.VMEM((owners * rows, sticks), F32)],
        "backward_z",
    )(recv, orb, slot, column, *zb)
    applied = applied.reshape(orbitals.shape)

    every = lax.all_gather(previous, "band")
    every = every.reshape(-1, 2, waves)
    sr, si = subspace[:, 0], subspace[:, 1]
    pr, pi = every[:, 0], every[:, 1]
    own = jnp.stack([dot_nt(sr, pr) + dot_nt(si, pi), dot_nt(sr, pi) - dot_nt(si, pr)])
    groups_of = lax.axis_size("band")
    tiles = own.reshape(2, own.shape[1], groups_of, bands)
    tiles = lax.all_to_all(jnp.moveaxis(tiles, 2, 0), "band", 0, 0, tiled=True)
    tiles = jnp.moveaxis(tiles, 1, 2).reshape(-1, 2, bands)
    tiles = lax.all_to_all(tiles[:, None], "fft", 0, 1, tiled=True)
    intersection = jnp.moveaxis(jnp.sum(tiles, axis=1), 0, 1)
    return applied, intersection


def solution(mesh):
    return jax.shard_map(
        per_device,
        mesh=mesh,
        in_specs=(
            P("band", None, "fft"),
            P("fft"),
            P("fft"),
            P("fft", None, None),
            P("band", None, "fft"),
            P("band", None, "fft"),
        ),
        out_specs=(P("band", None, "fft"), P(None, "fft", "band")),
        check_vma=False,
    )
```

```python
import functools
import math

import jax
import jax.numpy as jnp
import numpy as np
from jax import lax
from jax.experimental import pallas as pl
from jax.experimental.pallas import tpu as pltpu
from jax.sharding import PartitionSpec as P

F32 = jnp.float32
BF16 = jnp.bfloat16
NT = (((1,), (1,)), ((), ()))


def dot(a, b):
    return jnp.dot(a, b, preferred_element_type=F32)


def dot_nt(a, b):
    return lax.dot_general(a, b, NT, preferred_element_type=F32)


def tables(grid, owners):
    depth = grid // owners
    groups = owners // 4
    k = np.arange(grid)
    angle = 2.0 * math.pi * ((k[:, None] * k[None, :]) % grid) / grid
    cos, sin = np.cos(angle), np.sin(angle)
    icos, isin = cos / grid, -sin / grid
    zorder = np.arange(grid)
    zorder = (zorder % owners) * depth + zorder // owners
    rows = np.full(groups * 16, -1)
    for g in range(groups):
        rows[16 * g : 16 * g + 4 * depth] = 4 * depth * g + np.arange(4 * depth)

    def padded(table):
        out = np.zeros((groups * 16, grid))
        out[rows >= 0] = table[rows[rows >= 0]]
        return out

    def trio(c, s):
        return [jnp.asarray(t, BF16) for t in (c, s, -s)]

    zf = trio(cos[zorder], sin[zorder])
    zb = trio(icos[zorder], isin[zorder])
    yf = trio(cos, sin)
    yb = trio(icos, isin)
    xf = trio(padded(cos).T, padded(sin).T)
    xb = trio(padded(icos), padded(isin))
    return zf, zb, yf, yb, xf, xb


def vmem():
    return pl.BlockSpec(memory_space=pltpu.VMEM)


def hot(rows, index, kind=BF16):
    lanes = index.shape[1]
    return (lax.broadcasted_iota(jnp.int32, (rows, lanes), 0) == index).astype(F32).astype(kind)


def frequency(values, grid):
    return jnp.where(values >= grid // 2, values - grid, values).astype(F32)


def start_to(src, dst, send_sem, recv_sem, axis, peer):
    pltpu.make_async_remote_copy(
        src_ref=src,
        dst_ref=dst,
        send_sem=send_sem,
        recv_sem=recv_sem,
        device_id={axis: peer},
        device_id_type=pl.DeviceIdType.MESH,
    ).start()


def wait_bytes(ref, sem):
    pltpu.make_async_copy(ref, ref, sem).wait()


def others(axis, count, act):
    me = lax.axis_index(axis)

    def step(j, carry):
        act(me, lax.rem(me + j, count))
        return carry

    lax.fori_loop(1, count, step, 0)


def kernel(dims, *refs):
    owners, groups, grid, depth, sticks, waves, bands, teams, subs = dims
    orb, slot, column, pot, sub, prev = refs[:6]
    zf, zb, yf, yb, xf, xb = (refs[6 + 3 * i : 9 + 3 * i] for i in range(6))
    out, inter = refs[24:26]
    (stick_hot, plane_hot, rep, lhs, stage, send, recv, send2, recv2, cols, ymask, ymask_t, xmask,
     val, gre, gim, back, pall, r1, r2, r3) = refs[26:47]
    col_s, col_r, fwd_s, fwd_r, bwd_s, bwd_r, prev_s, prev_r, one_s, one_r, two_s, two_r = refs[47:]
    parts = 2 * bands
    wide = 4 * sticks
    chunk = 512
    me = lax.axis_index("fft")
    team = lax.axis_index("band")

    barrier = pltpu.get_barrier_semaphore()

    def greet(axis):
        def act(own, peer):
            pl.semaphore_signal(
                barrier, inc=1, device_id={axis: peer}, device_id_type=pl.DeviceIdType.MESH
            )

        return act

    others("fft", owners, greet("fft"))
    others("band", teams, greet("band"))

    for c in range(0, waves, chunk):
        cut = slice(c, c + chunk)
        sl = slot[:, cut]
        stick_hot[:, cut] = hot(sticks, lax.rem(sl, sticks))
        plane_hot[:, cut] = hot(grid, lax.div(sl, sticks))
        for r in range(parts):
            row = orb[r : r + 1, cut].astype(F32)
            rep[r, :, cut] = jnp.broadcast_to(row, (16, chunk)).astype(BF16)

    pl.semaphore_wait(barrier, owners + teams - 2)
    others("fft", owners, lambda own, peer: start_to(
        column, cols.at[own], col_s, col_r, "fft", peer))
    pltpu.make_async_copy(column, cols.at[me], col_r).start()
    others("band", teams, lambda own, peer: start_to(
        prev, pall.at[own], prev_s, prev_r, "band", peer))
    pltpu.make_async_copy(prev, pall.at[team], prev_r).start()

    zc, zs, zn = (t[...] for t in zf)
    for h in range(parts // 4):
        for r in range(4):
            lhs[sticks * r : sticks * (r + 1), :] = (
                stick_hot[...].reshape(sticks // 16, 16, waves) * rep[4 * h + r][None]
            ).reshape(sticks, waves)
        got = dot_nt(lhs[...], plane_hot[...]).astype(BF16)
        for k in range(2):
            b = 2 * h + k
            re = got[2 * k * sticks : (2 * k + 1) * sticks]
            im = got[(2 * k + 1) * sticks : (2 * k + 2) * sticks]
            pair = (
                dot_nt(zc, re) + dot_nt(zn, im),
                dot_nt(zs, re) + dot_nt(zc, im),
            )
            for p in range(2):
                for z in range(depth):
                    rows = pl.ds(p * bands + b, owners, stride=parts)
                    stage[z, rows, :] = pair[p][z * owners : (z + 1) * owners]
    for z in range(depth):
        for f in range(owners):
            send[z, f] = stage[z, parts * f : parts * (f + 1), :].astype(BF16)
    for z in range(depth):
        others("fft", owners, lambda own, peer, z=z: start_to(
            send.at[z, peer], recv.at[z, own], fwd_s.at[z], fwd_r.at[z], "fft", peer))
        pltpu.make_async_copy(send.at[z, me], recv.at[z, me], fwd_r.at[z]).start()

    wait_bytes(cols, col_r)
    for g in range(groups):
        for d in range(4):
            col = cols[4 * g + d]
            x = lax.div(col, grid)
            y = col - x * grid
            x = x - 4 * depth * g
            lanes = slice(sticks * d, sticks * (d + 1))
            ymask[g, :, lanes] = hot(grid, y)
            xmask[g, :, lanes] = hot(16, x, F32)
            yt = jnp.broadcast_to(y.astype(F32), (sticks, sticks)).T.astype(jnp.int32)
            wide_y = jnp.concatenate([yt, yt], axis=1)[:, :grid]
            ymask_t[g, lanes, :] = (
                lax.broadcasted_iota(jnp.int32, (sticks, grid), 1) == wide_y
            ).astype(F32).astype(BF16)

    wait_bytes(pall, prev_r)
    for t in range(teams):
        part = lax.dot_general(sub[...], pall[t], NT, preferred_element_type=F32)
        part = jnp.concatenate([part, jnp.zeros((2 * subs, 128 - parts), F32)], axis=1)
        for j in range(subs):
            r1[t, j] = part[2 * j : 2 * j + 2, :]
    others("band", teams, lambda own, peer: start_to(
        r1.at[peer], r2.at[own], one_s, one_r, "band", peer))
    pltpu.make_async_copy(r1.at[team], r2.at[team], one_r).start()

    def plane(z, carry):
        wait_bytes(recv.at[z], fwd_r.at[z])

        def scatter(g, carry):
            for d in range(4):
                val[g, :, sticks * d : sticks * (d + 1)] = recv[z, 4 * g + d].astype(F32)
            mask = xmask[g]
            block = jnp.concatenate(
                [(mask * val[g, r : r + 1, :]).astype(BF16) for r in range(parts)], axis=0
            )
            got = dot(block, ymask_t[g]).astype(BF16)
            at = pl.ds(pl.multiple_of(16 * g, 16), 16)
            gre[:, at, :] = got[: bands * 16].reshape(bands, 16, grid)
            gim[:, at, :] = got[bands * 16 :].reshape(bands, 16, grid)
            return carry

        lax.fori_loop(0, groups, scatter, 0, unroll=4)

        def local(b, carry):
            v = pot[z]
            re, im = gre[b], gim[b]
            yr = (dot(re, yf[0][...]) + dot(im, yf[2][...])).astype(BF16)
            yi = (dot(re, yf[1][...]) + dot(im, yf[0][...])).astype(BF16)
            wr = ((dot(xf[0][...], yr) + dot(xf[2][...], yi)) * v).astype(BF16)
            wi = ((dot(xf[1][...], yr) + dot(xf[0][...], yi)) * v).astype(BF16)
            br = (dot(xb[0][...], wr) + dot(xb[2][...], wi)).astype(BF16)
            bi = (dot(xb[1][...], wr) + dot(xb[0][...], wi)).astype(BF16)
            back[b] = (dot(br, yb[0][...]) + dot(bi, yb[2][...])).astype(BF16)
            back[bands + b] = (dot(br, yb[1][...]) + dot(bi, yb[0][...])).astype(BF16)
            return carry

        lax.fori_loop(0, bands, local, 0, unroll=2)

        def pick(g, carry):
            at = pl.ds(pl.multiple_of(16 * g, 16), 16)
            block = back[:, at, :].reshape(parts * 16, grid)
            t = dot(block, ymask[g]).reshape(parts, 16, wide)
            got = jnp.sum(t * xmask[g][None], axis=1)
            for d in range(4):
                send2[z, 4 * g + d] = got[:, sticks * d : sticks * (d + 1)].astype(BF16)
            return carry

        lax.fori_loop(0, groups, pick, 0, unroll=4)
        others("fft", owners, lambda own, peer: start_to(
            send2.at[z, peer], recv2.at[z, own], bwd_s.at[z], bwd_r.at[z], "fft", peer))
        pltpu.make_async_copy(send2.at[z, me], recv2.at[z, me], bwd_r.at[z]).start()
        return carry

    plane(0, 0)
    wait_bytes(r2, one_r)
    others("fft", owners, lambda own, peer: start_to(
        r2.at[lax.div(peer, subs), lax.rem(peer, subs)], r3.at[own], two_s, two_r, "fft", peer))
    pltpu.make_async_copy(
        r2.at[lax.div(me, subs), lax.rem(me, subs)], r3.at[me], two_r).start()
    lax.fori_loop(1, depth, plane, 0)

    wait_bytes(r3, two_r)
    total = jnp.sum(r3[...], axis=0)
    inter[...] = total

    col = column[...]
    x = lax.div(col, grid)
    y = col - x * grid
    coords = jnp.concatenate([x, y, x, y, x, y, x, y], axis=0).astype(F32).astype(BF16)
    for z in range(depth):
        wait_bytes(recv2.at[z], bwd_r.at[z])
        for f in range(owners):
            stage[z, parts * f : parts * (f + 1), :] = recv2[z, f].astype(F32)
    zc, zs, zn = (t[...] for t in zb)
    lines = []
    for b in range(bands):
        pair = []
        for p in range(2):
            rows = pl.ds(p * bands + b, owners, stride=parts)
            pair.append(
                jnp.concatenate([stage[z, rows, :] for z in range(depth)], axis=0).T.astype(BF16)
            )
        re, im = pair
        lines.append((dot(re, zc) + dot(im, zn)).astype(BF16))
        lines.append((dot(re, zs) + dot(im, zc)).astype(BF16))
    lines = jnp.concatenate(lines, axis=0)
    for c in range(0, waves, chunk):
        cut = slice(c, c + chunk)
        plane_at = lax.div(slot[:, cut], sticks)
        shot = stick_hot[:, cut]
        xy = dot(coords, shot)
        fz = frequency(plane_at, grid)
        fx = frequency(xy[0:1].astype(jnp.int32), grid)
        fy = frequency(xy[1:2].astype(jnp.int32), grid)
        kinetic = (fz * fz + fx * fx + fy * fy) * (2.0 / (grid * grid))
        t = dot(lines, plane_hot[:, cut]).reshape(parts, sticks, chunk)
        got = jnp.sum(t * shot.astype(F32)[None], axis=1)
        out[:, cut] = (got + kinetic * orb[:, cut].astype(F32)).astype(BF16)

    rest = pl.ds(0, owners - 1)
    for z in range(depth):
        wait_bytes(send.at[z, rest], fwd_s.at[z])
        wait_bytes(send2.at[z, rest], bwd_s.at[z])
    wait_bytes(cols.at[rest], col_s)
    wait_bytes(r3.at[rest], two_s)
    wait_bytes(pall.at[pl.ds(0, teams - 1)], prev_s)
    wait_bytes(r1.at[pl.ds(0, teams - 1)], one_s)


def per_device(orbitals, sphere_slot, stick_column, potential, subspace, previous):
    owners = lax.axis_size("fft")
    teams = lax.axis_size("band")
    groups = owners // 4
    depth, grid, _ = potential.shape
    sticks = stick_column.shape[0]
    waves = sphere_slot.shape[0]
    bands = orbitals.shape[0]
    subs = subspace.shape[0]
    parts = 2 * bands
    every = [t for trio in tables(grid, owners) for t in trio]
    dims = (owners, groups, grid, depth, sticks, waves, bands, teams, subs)
    message = pltpu.VMEM((depth, owners, parts, sticks), BF16)
    sums = pltpu.VMEM((teams, subs, 2, 128), F32)
    one = pltpu.SemaphoreType.DMA
    several = pltpu.SemaphoreType.DMA((depth,))
    applied, inter = pl.pallas_call(
        functools.partial(kernel, dims),
        out_shape=[
            jax.ShapeDtypeStruct((parts, waves), BF16),
            jax.ShapeDtypeStruct((2, 128), F32),
        ],
        in_specs=[vmem() for _ in range(6 + len(every))],
        out_specs=[vmem(), vmem()],
        scratch_shapes=[
            pltpu.VMEM((sticks, waves), BF16),
            pltpu.VMEM((grid, waves), BF16),
            pltpu.VMEM((parts, 16, waves), BF16),
            pltpu.VMEM((4 * sticks, waves), BF16),
            pltpu.VMEM((depth, owners * parts, sticks), F32),
            message,
            message,
            message,
            message,
            pltpu.VMEM((owners, 1, sticks), jnp.int32),
            pltpu.VMEM((groups, grid, 4 * sticks), BF16),
            pltpu.VMEM((groups, 4 * sticks, grid), BF16),
            pltpu.VMEM((groups, 16, 4 * sticks), F32),
            pltpu.VMEM((groups, parts, 4 * sticks), F32),
            pltpu.VMEM((bands, groups * 16, grid), BF16),
            pltpu.VMEM((bands, groups * 16, grid), BF16),
            pltpu.VMEM((parts, groups * 16, grid), BF16),
            pltpu.VMEM((teams, parts, waves), BF16),
            sums,
            sums,
            pltpu.VMEM((owners, 2, 128), F32),
            one, one, several, several, several, several, one, one, one, one, one, one,
        ],
        compiler_params=pltpu.CompilerParams(
            vmem_limit_bytes=60 * 2**20, collective_id=0, has_side_effects=True
        ),
        name="apply",
    )(
        orbitals.reshape(parts, waves),
        sphere_slot.reshape(1, waves),
        stick_column.reshape(1, sticks),
        potential,
        subspace.reshape(2 * subs, waves),
        previous.reshape(parts, waves),
        *every,
    )
    sums = inter[:, :parts].reshape(2, bands, 2)
    intersection = jnp.stack(
        [sums[0, :, 0] + sums[1, :, 1], sums[0, :, 1] - sums[1, :, 0]]
    )[:, None]
    return applied.reshape(orbitals.shape), intersection


def solution(mesh):
    return jax.shard_map(
        per_device,
        mesh=mesh,
        in_specs=(
            P("band", None, "fft"),
            P("fft"),
            P("fft"),
            P("fft", None, None),
            P("band", None, "fft"),
            P("band", None, "fft"),
        ),
        out_specs=(P("band", None, "fft"), P(None, "fft", "band")),
        check_vma=False,
    )
```

```python
import functools
import math

import jax
import jax.numpy as jnp
import numpy as np
from jax import lax
from jax.experimental import pallas as pl
from jax.experimental.pallas import tpu as pltpu
from jax.sharding import PartitionSpec as P

F32 = jnp.float32
BF16 = jnp.bfloat16
NT = (((1,), (1,)), ((), ()))


def dot(a, b):
    return jnp.dot(a, b, preferred_element_type=F32)


def dot_nt(a, b):
    return lax.dot_general(a, b, NT, preferred_element_type=F32)


def tables(grid, owners):
    depth = grid // owners
    block = 4 * depth
    half = grid // 2
    lanes = 128
    k = np.arange(grid)
    m = np.arange(half)
    zorder = (k % owners) * depth + k // owners

    def bf16(t):
        return jnp.asarray(t, BF16)

    def waves(rows, cols, sign, scale):
        angle = 2.0 * math.pi * ((rows[:, None] * cols[None, :]) % grid) / grid
        return np.cos(angle) * scale, sign * np.sin(angle) * scale

    def joined(c, s, rows, cols, height, width):
        out = np.zeros((2 * height, 2 * width))
        out[np.ix_(rows, cols)] = c
        out[np.ix_(height + rows, cols)] = -s
        out[np.ix_(rows, width + cols)] = s
        out[np.ix_(height + rows, width + cols)] = c
        return out

    xpos = 16 * (m // block) + m % block
    wide = groups16(owners) // 2
    order = np.concatenate([k[0::2], k[1::2]])
    zf = waves(zorder, order, 1.0, 1.0)
    zb = waves(order, zorder, -1.0, 1.0 / grid)
    made = [np.concatenate([zf[0], -zf[1]], 1), np.concatenate([zf[1], zf[0]], 1)]
    made += [np.concatenate([zb[0], -zb[1]], 1), np.concatenate([zb[1], zb[0]], 1)]
    for odd in range(2):
        made.append(joined(*waves(m, 2 * m + odd, 1.0, 1.0), m, m, lanes, lanes))
    for odd in range(2):
        made.append(joined(*waves(m, 2 * m + odd, 1.0, 1.0), xpos, m, wide, half).T)
    for odd in range(2):
        made.append(joined(*waves(2 * m + odd, m, -1.0, 1.0 / grid), m, xpos, half, wide).T)
    for odd in range(2):
        made.append(joined(*waves(2 * m + odd, m, -1.0, 1.0 / grid), m, m, lanes, lanes))
    return [bf16(t) for t in made]


def groups16(owners):
    return owners // 4 * 16


def vmem():
    return pl.BlockSpec(memory_space=pltpu.VMEM)


def hot(rows, index, kind=BF16):
    lanes = index.shape[1]
    return (lax.broadcasted_iota(jnp.int32, (rows, lanes), 0) == index).astype(F32).astype(kind)


def frequency(values, grid):
    return jnp.where(values >= grid // 2, values - grid, values).astype(F32)


def start_to(src, dst, send_sem, recv_sem, axis, peer):
    pltpu.make_async_remote_copy(
        src_ref=src,
        dst_ref=dst,
        send_sem=send_sem,
        recv_sem=recv_sem,
        device_id={axis: peer},
        device_id_type=pl.DeviceIdType.MESH,
    ).start()


def wait_bytes(ref, sem):
    pltpu.make_async_copy(ref, ref, sem).wait()


def others(axis, count, act):
    me = lax.axis_index(axis)

    def step(j, carry):
        act(me, lax.rem(me + j, count))
        return carry

    lax.fori_loop(1, count, step, 0, unroll=3)


def kernel(dims, *refs):
    owners, groups, grid, depth, sticks, waves, bands, teams, subs = dims
    orb, slot, column, pot, sub, prev = refs[:6]
    zf, zb, yf, xf, xb, yb = (refs[6 + 2 * i : 8 + 2 * i] for i in range(6))
    out, inter = refs[18:20]
    (high_hot, low_hot, rep, stage, send, recv, send2, recv2, cols, ymask, ymask_t, xmask,
     val, gre, gim, back, pots, turn, pall, r1, r2, r3) = refs[20:42]
    col_s, col_r, fwd_s, fwd_r, bwd_s, bwd_r, prev_s, prev_r, one_s, one_r, two_s, two_r = refs[42:]
    parts = 2 * bands
    wide = 4 * sticks
    half = grid // 2
    low = 2 * sticks
    rows = groups * 16
    mid = rows // 2
    chunk = 512
    me = lax.axis_index("fft")
    team = lax.axis_index("band")

    barrier = pltpu.get_barrier_semaphore()

    def greet(axis):
        def act(own, peer):
            pl.semaphore_signal(
                barrier, inc=1, device_id={axis: peer}, device_id_type=pl.DeviceIdType.MESH
            )

        return act

    others("fft", owners, greet("fft"))
    others("band", teams, greet("band"))

    with jax.named_scope("hots"):
        for c in range(0, waves, chunk):
            cut = slice(c, c + chunk)
            sl = slot[:, cut]
            high_hot[:, cut] = hot(half, lax.div(sl, low))
            low_hot[:, cut] = hot(low, lax.rem(sl, low))
            for b in range(bands):
                pair = orb[b, :, cut].astype(F32)
                for p in range(2):
                    rep[2 * b + p, :, cut] = jnp.broadcast_to(pair[p : p + 1], (16, chunk)).astype(BF16)

    with jax.named_scope("barrier"):
        pl.semaphore_wait(barrier, owners + teams - 2)
        others("fft", owners, lambda own, peer: start_to(
            column, cols.at[own], col_s, col_r, "fft", peer))
        pltpu.make_async_copy(column, cols.at[me], col_r).start()
        others("band", teams, lambda own, peer: start_to(
            prev, pall.at[own], prev_s, prev_r, "band", peer))
        pltpu.make_async_copy(prev, pall.at[team], prev_r).start()

    with jax.named_scope("zdft"):
        got = None
        for c in range(0, waves, chunk):
            cut = slice(c, c + chunk)
            high = high_hot[:, cut].reshape(half // 16, 16, chunk)
            block = jnp.concatenate(
                [(high * rep[r, :, cut][None]).reshape(half, chunk) for r in range(parts)], axis=0
            )
            piece = dot_nt(block, low_hot[:, cut])
            got = piece if got is None else got + piece
        got = got.astype(BF16)
        for b in range(bands):
            cut = got[2 * b * half : 2 * (b + 1) * half]
            field = jnp.concatenate(
                [cut[p * half : (p + 1) * half, q * sticks : (q + 1) * sticks]
                 for p in range(2) for q in range(2)], axis=0
            )
            for p in range(2):
                done = dot(zf[p][...], field)
                for z in range(depth):
                    at = pl.ds(p * bands + b, owners, stride=parts)
                    stage[z, at, :] = done[z * owners : (z + 1) * owners]
        for z in range(depth):
            for f in range(owners):
                send[z, f] = stage[z, parts * f : parts * (f + 1), :].astype(BF16)
    with jax.named_scope("sends"):
        for z in range(depth):
            others("fft", owners, lambda own, peer, z=z: start_to(
                send.at[z, peer], recv.at[z, own], fwd_s.at[z], fwd_r.at[z], "fft", peer))
            pltpu.make_async_copy(send.at[z, me], recv.at[z, me], fwd_r.at[z]).start()

    with jax.named_scope("masks"):
        wait_bytes(cols, col_r)
        for g in range(groups):
            for d in range(4):
                col = cols[4 * g + d]
                x = lax.div(col, grid)
                y = col - x * grid
                x = x - 4 * depth * g
                y = jnp.where(y >= half, y + (128 - half), y)
                lanes = slice(sticks * d, sticks * (d + 1))
                ymask[g, :, lanes] = hot(256, y)
                xmask[g, :, lanes] = hot(16, x, F32)
                yt = jnp.broadcast_to(y.astype(F32), (sticks, sticks)).T.astype(jnp.int32)
                wide_y = jnp.concatenate([yt, yt], axis=1)
                ymask_t[g, lanes, :] = (
                    lax.broadcasted_iota(jnp.int32, (sticks, 256), 1) == wide_y
                ).astype(F32).astype(BF16)
        side = jnp.zeros((grid, 256 - grid), F32)
        gap = jnp.zeros((128 - half, 256), F32)

        def sorted_rows(table):
            for q in range(2):
                turn[q] = table[:, 128 * q : 128 * (q + 1)]
            return [
                jnp.concatenate([turn[q, pl.ds(odd, half, stride=2), :] for q in range(2)], axis=1)
                for odd in range(2)
            ]

        for z in range(depth):
            even, odd = sorted_rows(jnp.concatenate([pot[z], side], axis=1))
            table = jnp.concatenate([even, odd], axis=0).T[:grid]
            even, odd = sorted_rows(jnp.concatenate([table, side], axis=1))
            pots[z] = jnp.concatenate([even, gap, odd, gap], axis=0).T[:grid]

    with jax.named_scope("inter1"):
        wait_bytes(pall, prev_r)
        left = jnp.concatenate([sub[j] for j in range(subs)], axis=0)
        for t in range(teams):
            right = jnp.concatenate(
                [pall[t, i][p : p + 1] for p in range(2) for i in range(bands)], axis=0
            )
            part = dot_nt(left, right)
            part = jnp.concatenate([part, jnp.zeros((2 * subs, 128 - parts), F32)], axis=1)
            for j in range(subs):
                r1[t, j] = part[2 * j : 2 * j + 2, :]
        others("band", teams, lambda own, peer: start_to(
            r1.at[peer], r2.at[own], one_s, one_r, "band", peer))
        pltpu.make_async_copy(r1.at[team], r2.at[team], one_r).start()

    def plane(z, carry):
        with jax.named_scope("waitz"):
            wait_bytes(recv.at[z], fwd_r.at[z])

        def scatter(g, carry):
            for d in range(4):
                val[g, :, sticks * d : sticks * (d + 1)] = recv[z, 4 * g + d].astype(F32)
            mask = xmask[g]
            block = jnp.concatenate(
                [(mask * val[g, r : r + 1, :]).astype(BF16) for r in range(parts)], axis=0
            )
            got = dot(block, ymask_t[g]).astype(BF16)
            at = pl.ds(pl.multiple_of(16 * g, 16), 16)
            gre[:, at, :] = got[: bands * 16].reshape(bands, 16, 256)
            gim[:, at, :] = got[bands * 16 :].reshape(bands, 16, 256)
            return carry

        with jax.named_scope("scatter"):
            lax.fori_loop(0, groups, scatter, 0, unroll=4)

        with jax.named_scope("local"):
            local(z)

        def quarter(i, carry):
            q = lax.rem(lax.div(me, 16) + i, owners // 16)
            for k in range(4):
                g = 4 * q + k
                at = pl.ds(pl.multiple_of(16 * g, 16), 16)
                block = back[:, at, :].reshape(parts * 16, 256)
                t = dot(block, ymask[g]).reshape(parts, 16, wide)
                got = jnp.sum(t * xmask[g][None], axis=1)
                for d in range(4):
                    send2[z, 4 * g + d] = got[:, sticks * d : sticks * (d + 1)].astype(BF16)

            def give(j, carry):
                peer = 16 * q + lax.rem(me + j, 16)
                start_to(send2.at[z, peer], recv2.at[z, me], bwd_s.at[z], bwd_r.at[z], "fft", peer)
                return carry

            lax.fori_loop(1, 16, give, 0, unroll=5)

            @pl.when(i > 0)
            def _():
                give(0, 0)

            @pl.when(i == 0)
            def _():
                pltpu.make_async_copy(send2.at[z, me], recv2.at[z, me], bwd_r.at[z]).start()

            return carry

        with jax.named_scope("pick"):
            lax.fori_loop(0, owners // 16, quarter, 0)
        return carry

    def local(z):
        ve, vo = pots[z, :half], pots[z, half:]
        every = range(bands)
        ys = []
        for b in every:
            re, im = gre[b], gim[b]
            a = jnp.concatenate([re[:, :128], im[:, :128]], axis=1)
            c = jnp.concatenate([re[:, 128:], im[:, 128:]], axis=1)
            ys.append((dot(a + c, yf[0][...]).astype(BF16), dot(a - c, yf[1][...]).astype(BF16)))
        xs = []
        for b in every:
            e, o = ys[b]
            re = jnp.concatenate([e[:, :128], o[:, :128]], axis=1)
            im = jnp.concatenate([e[:, 128:], o[:, 128:]], axis=1)
            a = jnp.concatenate([re[:mid], im[:mid]], axis=0)
            c = jnp.concatenate([re[mid:], im[mid:]], axis=0)
            we = (dot(xf[0][...], a + c) * jnp.concatenate([ve, ve], axis=0)).astype(BF16)
            wo = (dot(xf[1][...], a - c) * jnp.concatenate([vo, vo], axis=0)).astype(BF16)
            xs.append((we, wo))
        bs = []
        for b in every:
            e = dot(xb[0][...], xs[b][0])
            o = dot(xb[1][...], xs[b][1])
            bs.append(((e + o).astype(BF16), (e - o).astype(BF16)))
        for b in every:
            p, m = bs[b]
            re = jnp.concatenate([p[:mid], m[:mid]], axis=0)
            im = jnp.concatenate([p[mid:], m[mid:]], axis=0)
            e = dot(jnp.concatenate([re[:, :128], im[:, :128]], axis=1), yb[0][...])
            o = dot(jnp.concatenate([re[:, 128:], im[:, 128:]], axis=1), yb[1][...])
            p, m = (e + o).astype(BF16), (e - o).astype(BF16)
            back[b] = jnp.concatenate([p[:, :128], m[:, :128]], axis=1)
            back[bands + b] = jnp.concatenate([p[:, 128:], m[:, 128:]], axis=1)

    lax.fori_loop(0, depth, plane, 0)

    with jax.named_scope("inter2"):
        wait_bytes(r2, one_r)
        others("fft", owners, lambda own, peer: start_to(
            r2.at[lax.div(peer, subs), lax.rem(peer, subs)], r3.at[own], two_s, two_r, "fft", peer))
        pltpu.make_async_copy(
            r2.at[lax.div(me, subs), lax.rem(me, subs)], r3.at[me], two_r).start()

    with jax.named_scope("waitback"):
        col = column[...]
        x = lax.div(col, grid)
        y = col - x * grid
        coords = jnp.concatenate([x, y, x, y, x, y, x, y], axis=0).astype(F32).astype(BF16)
        coords = jnp.concatenate([coords, coords], axis=1)
        for z in range(depth):
            wait_bytes(recv2.at[z], bwd_r.at[z])
            for f in range(owners):
                stage[z, parts * f : parts * (f + 1), :] = recv2[z, f].astype(F32)
    with jax.named_scope("zback"):
        lines = []
        for b in range(bands):
            field = jnp.concatenate(
                [stage[z, pl.ds(p * bands + b, owners, stride=parts), :].astype(BF16)
                 for p in range(2) for z in range(depth)], axis=0
            )
            for p in range(2):
                done = dot(zb[p][...], field).astype(BF16)
                lines.append(jnp.concatenate([done[:half], done[half:]], axis=1))
        lines = jnp.concatenate(lines, axis=0)
    with jax.named_scope("pickw"):
        for c in range(0, waves, chunk):
            cut = slice(c, c + chunk)
            plane_at = lax.div(slot[:, cut], sticks)
            low_cut = low_hot[:, cut]
            xy = dot(coords, low_cut)
            fz = frequency(plane_at, grid)
            fx = frequency(xy[0:1].astype(jnp.int32), grid)
            fy = frequency(xy[1:2].astype(jnp.int32), grid)
            kinetic = (fz * fz + fx * fx + fy * fy) * (2.0 / (grid * grid))
            t = dot(lines, low_cut).reshape(parts, half, chunk)
            got = jnp.sum(t * high_hot[:, cut].astype(F32)[None], axis=1)
            for b in range(bands):
                out[b, :, cut] = (
                    got[2 * b : 2 * b + 2] + kinetic * orb[b, :, cut].astype(F32)
                ).astype(BF16)

    with jax.named_scope("waits"):
        wait_bytes(r3, two_r)
        total = jnp.sum(r3[...], axis=0)
        moved = pltpu.roll(total, 128 - bands, 1)
        inter[0] = (total[0:1] + moved[1:2])[:, :bands]
        inter[1] = (moved[0:1] - total[1:2])[:, :bands]
        rest = pl.ds(0, owners - 1)
        for z in range(depth):
            wait_bytes(send.at[z, rest], fwd_s.at[z])
            wait_bytes(send2.at[z, rest], bwd_s.at[z])
        wait_bytes(cols.at[rest], col_s)
        wait_bytes(r3.at[rest], two_s)
        wait_bytes(pall.at[pl.ds(0, teams - 1)], prev_s)
        wait_bytes(r1.at[pl.ds(0, teams - 1)], one_s)


def per_device(orbitals, sphere_slot, stick_column, potential, subspace, previous):
    owners = lax.axis_size("fft")
    teams = lax.axis_size("band")
    groups = owners // 4
    depth, grid, _ = potential.shape
    sticks = stick_column.shape[0]
    waves = sphere_slot.shape[0]
    bands = orbitals.shape[0]
    subs = subspace.shape[0]
    parts = 2 * bands
    half = grid // 2
    every = tables(grid, owners)
    dims = (owners, groups, grid, depth, sticks, waves, bands, teams, subs)
    message = pltpu.VMEM((depth, owners, parts, sticks), BF16)
    sums = pltpu.VMEM((teams, subs, 2, 128), F32)
    one = pltpu.SemaphoreType.DMA
    several = pltpu.SemaphoreType.DMA((depth,))
    return tuple(pl.pallas_call(
        functools.partial(kernel, dims),
        out_shape=[
            jax.ShapeDtypeStruct(orbitals.shape, BF16),
            jax.ShapeDtypeStruct((2, 1, bands), F32),
        ],
        in_specs=[vmem() for _ in range(6 + len(every))],
        out_specs=[vmem(), vmem()],
        scratch_shapes=[
            pltpu.VMEM((half, waves), BF16),
            pltpu.VMEM((2 * sticks, waves), BF16),
            pltpu.VMEM((parts, 16, waves), BF16),
            pltpu.VMEM((depth, owners * parts, sticks), F32),
            message,
            message,
            message,
            message,
            pltpu.VMEM((owners, 1, sticks), jnp.int32),
            pltpu.VMEM((groups, 256, 4 * sticks), BF16),
            pltpu.VMEM((groups, 4 * sticks, 256), BF16),
            pltpu.VMEM((groups, 16, 4 * sticks), F32),
            pltpu.VMEM((groups, parts, 4 * sticks), F32),
            pltpu.VMEM((bands, groups * 16, 256), BF16),
            pltpu.VMEM((bands, groups * 16, 256), BF16),
            pltpu.VMEM((parts, groups * 16, 256), BF16),
            pltpu.VMEM((depth, grid, 256), F32),
            pltpu.VMEM((2, grid, 128), F32),
            pltpu.VMEM((teams, *previous.shape), BF16),
            sums,
            sums,
            pltpu.VMEM((owners, 2, 128), F32),
            one, one, several, several, several, several, one, one, one, one, one, one,
        ],
        compiler_params=pltpu.CompilerParams(
            vmem_limit_bytes=60 * 2**20, collective_id=0, has_side_effects=True
        ),
        name="apply",
    )(
        orbitals,
        sphere_slot.reshape(1, waves),
        stick_column.reshape(1, sticks),
        potential,
        subspace,
        previous,
        *every,
    ))


def solution(mesh):
    return jax.shard_map(
        per_device,
        mesh=mesh,
        in_specs=(
            P("band", None, "fft"),
            P("fft"),
            P("fft"),
            P("fft", None, None),
            P("band", None, "fft"),
            P("band", None, "fft"),
        ),
        out_specs=(P("band", None, "fft"), P(None, "fft", "band")),
        check_vma=False,
    )
```

```python
import functools
import math

import jax
import jax.numpy as jnp
import numpy as np
from jax import lax
from jax.experimental import pallas as pl
from jax.experimental.pallas import tpu as pltpu
from jax.sharding import PartitionSpec as P

F32 = jnp.float32
BF16 = jnp.bfloat16
NT = (((1,), (1,)), ((), ()))


def dot(a, b):
    return jnp.dot(a, b, preferred_element_type=F32)


def dot_nt(a, b):
    return lax.dot_general(a, b, NT, preferred_element_type=F32)


def tables(grid, owners):
    depth = grid // owners
    block = 4 * depth
    half = grid // 2
    lanes = 128
    k = np.arange(grid)
    m = np.arange(half)
    zorder = (k % owners) * depth + k // owners

    def bf16(t):
        return jnp.asarray(t, BF16)

    def waves(rows, cols, sign, scale):
        angle = 2.0 * math.pi * ((rows[:, None] * cols[None, :]) % grid) / grid
        return np.cos(angle) * scale, sign * np.sin(angle) * scale

    def joined(c, s, rows, cols, height, width):
        out = np.zeros((2 * height, 2 * width))
        out[np.ix_(rows, cols)] = c
        out[np.ix_(height + rows, cols)] = -s
        out[np.ix_(rows, width + cols)] = s
        out[np.ix_(height + rows, width + cols)] = c
        return out

    xpos = 16 * (m // block) + m % block
    wide = groups16(owners) // 2
    order = np.concatenate([k[0::2], k[1::2]])
    zf = waves(zorder, order, 1.0, 1.0)
    zb = waves(order, zorder, -1.0, 1.0 / grid)
    made = [np.concatenate([zf[0], -zf[1]], 1), np.concatenate([zf[1], zf[0]], 1)]
    made += [np.concatenate([zb[0], -zb[1]], 1), np.concatenate([zb[1], zb[0]], 1)]
    for odd in range(2):
        made.append(joined(*waves(m, 2 * m + odd, 1.0, 1.0), m, m, lanes, lanes))
    for odd in range(2):
        made.append(joined(*waves(m, 2 * m + odd, 1.0, 1.0), xpos, m, wide, half).T)
    for odd in range(2):
        made.append(joined(*waves(2 * m + odd, m, -1.0, 1.0 / grid), m, xpos, half, wide).T)
    for odd in range(2):
        made.append(joined(*waves(2 * m + odd, m, -1.0, 1.0 / grid), m, m, lanes, lanes))
    return [bf16(t) for t in made]


def groups16(owners):
    return owners // 4 * 16


def vmem():
    return pl.BlockSpec(memory_space=pltpu.VMEM)


def hot(count, index, numbers):
    lanes = index.shape[1]
    index = jnp.broadcast_to(index.astype(F32), (16, lanes)).astype(BF16)
    rows = numbers[:count].reshape(count // 16, 16, numbers.shape[1])
    rows = jnp.concatenate([rows] * (lanes // numbers.shape[1]), axis=2)
    one, zero = jnp.ones((), BF16), jnp.zeros((), BF16)
    return jnp.where(rows == index[None], one, zero).reshape(count, lanes)


def frequency(values, grid):
    return jnp.where(values >= grid // 2, values - grid, values).astype(F32)


def start_to(src, dst, send_sem, recv_sem, axis, peer):
    pltpu.make_async_remote_copy(
        src_ref=src,
        dst_ref=dst,
        send_sem=send_sem,
        recv_sem=recv_sem,
        device_id={axis: peer},
        device_id_type=pl.DeviceIdType.MESH,
    ).start()


def wait_bytes(ref, sem):
    pltpu.make_async_copy(ref, ref, sem).wait()


def others(axis, count, act):
    me = lax.axis_index(axis)
    skip = count // 2 + count // 8 + 1

    def step(j, carry):
        act(me, lax.rem(me + skip * j, count))
        return carry

    lax.fori_loop(1, count, step, 0, unroll=3)


def near(step):
    return lax.rem(lax.div(step * (step + 1), 2), 4)


def kernel(dims, *refs):
    owners, groups, grid, depth, sticks, waves, bands, teams, subs = dims
    inputs, (out, inter), refs = refs[:18], refs[18:20], refs[20:]
    prev = inputs[5]
    held, refs = refs[:17], refs[17:]
    orb, slot, column, pot, sub = held[:5]
    zf, zb, yf, xf, xb, yb = (held[5 + 2 * i : 7 + 2 * i] for i in range(6))
    (high_hot, low_hot, rep, stage, send, recv, send2, recv2, cols, ymask, ymask_t, xmask,
     val, gre, gim, back, pots, turn, left, numbers, pall, r1, r2, r3) = refs[:24]
    (in_s, col_s, col_r, fwd_s, first_r, fwd_r, bwd_s, bwd_r, prev_s, prev_r,
     one_s, one_r, two_s, two_r) = refs[24:]
    parts = 2 * bands
    wide = 4 * sticks
    half = grid // 2
    low = 2 * sticks
    rows = groups * 16
    mid = rows // 2
    chunk = 512
    me = lax.axis_index("fft")
    team = lax.axis_index("band")
    batch = lax.div(lax.rem(me, 16), 4)
    within = 4 * lax.div(me, 16) + lax.rem(me, 4)
    place = 16 * batch + within

    barrier = pltpu.get_barrier_semaphore()

    def greet(axis):
        def act(own, peer):
            pl.semaphore_signal(
                barrier, inc=1, device_id={axis: peer}, device_id_type=pl.DeviceIdType.MESH
            )

        return act

    given = [*inputs[:5], *inputs[6:]]
    fetches = [
        pltpu.make_async_copy(src, dst, in_s.at[i])
        for i, (src, dst) in enumerate(zip(given, held, strict=True))
    ]
    for i in (1, 0, 2, 5, 6):
        fetches[i].start()
    others("fft", owners, greet("fft"))
    others("band", teams, greet("band"))
    for i in (3, 4, *range(7, 17)):
        fetches[i].start()

    with jax.named_scope("hots"):
        numbers[...] = lax.broadcasted_iota(jnp.int32, (256, 128), 0).astype(F32).astype(BF16)
        for i in (0, 1, 2):
            fetches[i].wait()
        for c in range(0, waves, chunk):
            cut = slice(c, c + chunk)
            sl = slot[:, cut]
            high_hot[:, cut] = hot(half, lax.div(sl, low), numbers[...])
            low_hot[:, cut] = hot(low, lax.rem(sl, low), numbers[...])
            for b in range(bands):
                pair = orb[b, :, cut].astype(F32)
                for p in range(2):
                    rep[2 * b + p, :, cut] = jnp.broadcast_to(pair[p : p + 1], (16, chunk)).astype(BF16)

    with jax.named_scope("zdft"):
        got = None
        for c in range(0, waves, chunk):
            cut = slice(c, c + chunk)
            high = high_hot[:, cut].reshape(half // 16, 16, chunk)
            block = jnp.concatenate(
                [(high * rep[r, :, cut][None]).reshape(half, chunk) for r in range(parts)], axis=0
            )
            piece = dot_nt(block, low_hot[:, cut])
            got = piece if got is None else got + piece
        got = got.astype(BF16)
        for i in (5, 6):
            fetches[i].wait()
        for b in range(bands):
            cut = got[2 * b * half : 2 * (b + 1) * half]
            field = jnp.concatenate(
                [cut[p * half : (p + 1) * half, q * sticks : (q + 1) * sticks]
                 for p in range(2) for q in range(2)], axis=0
            )
            for p in range(2):
                done = dot(zf[p][...], field)
                for z in range(depth):
                    at = pl.ds(p * bands + b, owners, stride=parts)
                    stage[z, at, :] = done[z * owners : (z + 1) * owners]
        for z in range(depth):
            for f in range(owners):
                send[z, f] = stage[z, parts * f : parts * (f + 1), :].astype(BF16)

    with jax.named_scope("early"):
        for i in (3, 4, *range(7, 17)):
            fetches[i].wait()
        side = jnp.zeros((grid, 256 - grid), F32)
        gap = jnp.zeros((128 - half, 256), F32)

        def sorted_rows(table):
            for q in range(2):
                turn[q] = table[:, 128 * q : 128 * (q + 1)]
            return [
                jnp.concatenate([turn[q, pl.ds(odd, half, stride=2), :] for q in range(2)], axis=1)
                for odd in range(2)
            ]

        for z in range(depth):
            even, odd = sorted_rows(jnp.concatenate([pot[z], side], axis=1))
            table = jnp.concatenate([even, odd], axis=0).T[:grid]
            even, odd = sorted_rows(jnp.concatenate([table, side], axis=1))
            pots[z] = jnp.concatenate([even, gap, odd, gap], axis=0).T[:grid]
        left[...] = jnp.concatenate([sub[j] for j in range(subs)], axis=0)

    with jax.named_scope("barrier"):
        pl.semaphore_wait(barrier, owners + teams - 2)
    with jax.named_scope("sends"):
        others("fft", owners, lambda own, peer: start_to(
            column, cols.at[place], col_s, col_r.at[batch], "fft", peer))
        pltpu.make_async_copy(column, cols.at[place], col_r.at[batch]).start()
        others("fft", owners, lambda own, peer: start_to(
            send.at[0, peer], recv.at[0, place], fwd_s.at[0], first_r.at[batch], "fft", peer))
        pltpu.make_async_copy(send.at[0, me], recv.at[0, place], first_r.at[batch]).start()
        for z in range(1, depth):
            others("fft", owners, lambda own, peer, z=z: start_to(
                send.at[z, peer], recv.at[z, place], fwd_s.at[z], fwd_r.at[z], "fft", peer))
            pltpu.make_async_copy(send.at[z, me], recv.at[z, place], fwd_r.at[z]).start()
        others("band", teams, lambda own, peer: start_to(
            prev, pall.at[own], prev_s, prev_r, "band", peer))
        pltpu.make_async_copy(prev, pall.at[team], prev_r).start()

    def masks(h):
        g = 4 * lax.rem(h, 4) + lax.div(h, 4)
        for d in range(4):
            col = cols[4 * h + d]
            x = lax.div(col, grid)
            y = col - x * grid
            x = x - 4 * depth * g
            y = jnp.where(y >= half, y + (128 - half), y)
            lanes = slice(sticks * d, sticks * (d + 1))
            ymask[h, :, lanes] = hot(256, y, numbers[...])
            xmask[h, :, lanes] = hot(16, x, numbers[...])
            yt = jnp.broadcast_to(y.astype(F32), (sticks, sticks)).T.astype(BF16)
            line = lax.broadcasted_iota(jnp.int32, (16, 128), 1).astype(F32)
            one, zero = jnp.ones((), BF16), jnp.zeros((), BF16)
            for q in range(2):
                at = (line + 128.0 * q).astype(BF16)[None]
                same = yt.reshape(sticks // 16, 16, 128) == at
                ymask_t[h, lanes, 128 * q : 128 * (q + 1)] = jnp.where(same, one, zero).reshape(sticks, 128)

    def scatter(z, h):
        for d in range(4):
            val[h, :, sticks * d : sticks * (d + 1)] = recv[z, 4 * h + d].astype(F32)
        mask = xmask[h]
        block = jnp.concatenate(
            [mask * jnp.broadcast_to(val[h, r : r + 1, :], (16, wide)).astype(BF16)
             for r in range(parts)], axis=0
        )
        got = dot(block, ymask_t[h]).astype(BF16)
        g = 4 * lax.rem(h, 4) + lax.div(h, 4)
        at = pl.ds(pl.multiple_of(16 * g, 16), 16)
        gre[:, at, :] = got[: bands * 16].reshape(bands, 16, 256)
        gim[:, at, :] = got[bands * 16 :].reshape(bands, 16, 256)

    def local(z):
        ve, vo = pots[z, :half], pots[z, half:]
        every = range(bands)
        ys = []
        for b in every:
            re, im = gre[b], gim[b]
            a = jnp.concatenate([re[:, :128], im[:, :128]], axis=1)
            c = jnp.concatenate([re[:, 128:], im[:, 128:]], axis=1)
            ys.append((dot(a + c, yf[0][...]).astype(BF16), dot(a - c, yf[1][...]).astype(BF16)))
        xs = []
        for b in every:
            e, o = ys[b]
            re = jnp.concatenate([e[:, :128], o[:, :128]], axis=1)
            im = jnp.concatenate([e[:, 128:], o[:, 128:]], axis=1)
            a = jnp.concatenate([re[:mid], im[:mid]], axis=0)
            c = jnp.concatenate([re[mid:], im[mid:]], axis=0)
            we = (dot(xf[0][...], a + c) * jnp.concatenate([ve, ve], axis=0)).astype(BF16)
            wo = (dot(xf[1][...], a - c) * jnp.concatenate([vo, vo], axis=0)).astype(BF16)
            xs.append((we, wo))
        bs = []
        for b in every:
            e = dot(xb[0][...], xs[b][0])
            o = dot(xb[1][...], xs[b][1])
            bs.append(((e + o).astype(BF16), (e - o).astype(BF16)))
        for b in every:
            p, m = bs[b]
            re = jnp.concatenate([p[:mid], m[:mid]], axis=0)
            im = jnp.concatenate([p[mid:], m[mid:]], axis=0)
            e = dot(jnp.concatenate([re[:, :128], im[:, :128]], axis=1), yb[0][...])
            o = dot(jnp.concatenate([re[:, 128:], im[:, 128:]], axis=1), yb[1][...])
            p, m = (e + o).astype(BF16), (e - o).astype(BF16)
            back[b] = jnp.concatenate([p[:, :128], m[:, :128]], axis=1)
            back[bands + b] = jnp.concatenate([p[:, 128:], m[:, 128:]], axis=1)

    def quarter(z, i):
        q = lax.rem(batch + near(3 - i), 4)
        line = lax.broadcasted_iota(jnp.int32, (16, parts * 16), 1)
        row = lax.broadcasted_iota(jnp.int32, (16, parts * 16), 0)
        ones = (lax.div(line, 16) == row).astype(F32).astype(BF16)
        for k in range(4):
            h = 4 * q + k
            g = 4 * k + q
            at = pl.ds(pl.multiple_of(16 * g, 16), 16)
            block = back[:, at, :].reshape(parts * 16, 256)
            t = dot(block, ymask[h]).astype(BF16).reshape(parts, 16, wide)
            t = (t * xmask[h][None]).reshape(parts * 16, wide)
            got = dot(ones, t)[:parts]
            for d in range(4):
                send2[z, 4 * h + d] = got[:, sticks * d : sticks * (d + 1)].astype(BF16)

        def give(j, carry):
            t = lax.rem(within + 9 * j, 16)
            peer = 16 * lax.div(t, 4) + 4 * q + lax.rem(t, 4)
            start_to(send2.at[z, 16 * q + t], recv2.at[z, me], bwd_s.at[z], bwd_r.at[z], "fft", peer)
            return carry

        lax.fori_loop(1, 16, give, 0, unroll=5)

        @pl.when(i < 3)
        def _():
            give(0, 0)

        @pl.when(i == 3)
        def _():
            pltpu.make_async_copy(send2.at[z, place], recv2.at[z, me], bwd_r.at[z]).start()

    def work(z):
        with jax.named_scope("local"):
            local(z)

        def step(i, carry):
            quarter(z, i)
            return carry

        with jax.named_scope("pick"):
            lax.fori_loop(0, 4, step, 0)

    def first(i, carry):
        q = lax.rem(batch + near(i), 4)
        wait_bytes(cols.at[pl.ds(16 * q, 16)], col_r.at[q])
        for k in range(4):
            masks(4 * q + k)
        wait_bytes(recv.at[0, pl.ds(16 * q, 16)], first_r.at[q])
        for k in range(4):
            scatter(0, 4 * q + k)
        return carry

    with jax.named_scope("first"):
        lax.fori_loop(0, 4, first, 0)

    def plane(z, carry):
        @pl.when(z > 0)
        def _():
            wait_bytes(recv.at[z], fwd_r.at[z])

            def step(h, carry):
                scatter(z, h)
                return carry

            with jax.named_scope("scatter"):
                lax.fori_loop(0, groups, step, 0, unroll=8)

        work(z)

        @pl.when(z == 0)
        def _():
            with jax.named_scope("inter1"):
                wait_bytes(pall, prev_r)
                for t in range(teams):
                    right = jnp.concatenate(
                        [pall[t, i][p : p + 1] for p in range(2) for i in range(bands)], axis=0
                    )
                    part = dot_nt(left[...], right)
                    part = jnp.concatenate(
                        [part, jnp.zeros((2 * subs, 128 - parts), F32)], axis=1
                    )
                    for j in range(subs):
                        r1[t, j] = part[2 * j : 2 * j + 2, :]
                others("band", teams, lambda own, peer: start_to(
                    r1.at[peer], r2.at[own], one_s, one_r, "band", peer))
                pltpu.make_async_copy(r1.at[team], r2.at[team], one_r).start()

        return carry

    lax.fori_loop(0, depth, plane, 0)

    with jax.named_scope("inter2"):
        wait_bytes(r2, one_r)
        others("fft", owners, lambda own, peer: start_to(
            r2.at[lax.div(peer, subs), lax.rem(peer, subs)], r3.at[own], two_s, two_r, "fft", peer))
        pltpu.make_async_copy(
            r2.at[lax.div(me, subs), lax.rem(me, subs)], r3.at[me], two_r).start()

    with jax.named_scope("waitback"):
        col = column[...]
        x = lax.div(col, grid)
        y = col - x * grid
        coords = jnp.concatenate([x, y, x, y, x, y, x, y], axis=0).astype(F32).astype(BF16)
        coords = jnp.concatenate([coords, coords], axis=1)
        for z in range(depth):
            wait_bytes(recv2.at[z], bwd_r.at[z])
            for f in range(owners):
                stage[z, parts * f : parts * (f + 1), :] = recv2[z, f].astype(F32)
    with jax.named_scope("zback"):
        lines = []
        for b in range(bands):
            field = jnp.concatenate(
                [stage[z, pl.ds(p * bands + b, owners, stride=parts), :].astype(BF16)
                 for p in range(2) for z in range(depth)], axis=0
            )
            for p in range(2):
                done = dot(zb[p][...], field).astype(BF16)
                lines.append(jnp.concatenate([done[:half], done[half:]], axis=1))
        lines = jnp.concatenate(lines, axis=0)
    with jax.named_scope("pickw"):
        for c in range(0, waves, chunk):
            cut = slice(c, c + chunk)
            plane_at = lax.div(slot[:, cut], sticks)
            low_cut = low_hot[:, cut]
            xy = dot(coords, low_cut)
            fz = frequency(plane_at, grid)
            fx = frequency(xy[0:1].astype(jnp.int32), grid)
            fy = frequency(xy[1:2].astype(jnp.int32), grid)
            kinetic = (fz * fz + fx * fx + fy * fy) * (2.0 / (grid * grid))
            t = dot(lines, low_cut).reshape(parts, half, chunk)
            got = jnp.sum(t * high_hot[:, cut].astype(F32)[None], axis=1)
            for b in range(bands):
                out[b, :, cut] = (
                    got[2 * b : 2 * b + 2] + kinetic * orb[b, :, cut].astype(F32)
                ).astype(BF16)

    with jax.named_scope("waits"):
        wait_bytes(r3, two_r)
        total = jnp.sum(r3[...], axis=0)
        moved = pltpu.roll(total, 128 - bands, 1)
        inter[0] = (total[0:1] + moved[1:2])[:, :bands]
        inter[1] = (moved[0:1] - total[1:2])[:, :bands]
        rest = pl.ds(0, owners - 1)
        for z in range(depth):
            wait_bytes(send.at[z, rest], fwd_s.at[z])
            wait_bytes(send2.at[z, rest], bwd_s.at[z])
        wait_bytes(cols.at[rest], col_s)
        wait_bytes(r3.at[rest], two_s)
        wait_bytes(pall.at[pl.ds(0, teams - 1)], prev_s)
        wait_bytes(r1.at[pl.ds(0, teams - 1)], one_s)


def per_device(orbitals, sphere_slot, stick_column, potential, subspace, previous):
    owners = lax.axis_size("fft")
    teams = lax.axis_size("band")
    groups = owners // 4
    depth, grid, _ = potential.shape
    sticks = stick_column.shape[0]
    waves = sphere_slot.shape[0]
    bands = orbitals.shape[0]
    subs = subspace.shape[0]
    parts = 2 * bands
    half = grid // 2
    every = tables(grid, owners)
    given = [
        orbitals,
        sphere_slot.reshape(1, waves),
        stick_column.reshape(1, sticks),
        potential,
        subspace,
        previous,
        *every,
    ]
    dims = (owners, groups, grid, depth, sticks, waves, bands, teams, subs)
    message = pltpu.VMEM((depth, owners, parts, sticks), BF16)
    sums = pltpu.VMEM((teams, subs, 2, 128), F32)
    one = pltpu.SemaphoreType.DMA
    four = pltpu.SemaphoreType.DMA((4,))
    several = pltpu.SemaphoreType.DMA((depth,))
    return tuple(pl.pallas_call(
        functools.partial(kernel, dims),
        out_shape=[
            jax.ShapeDtypeStruct(orbitals.shape, BF16),
            jax.ShapeDtypeStruct((2, 1, bands), F32),
        ],
        in_specs=[pl.BlockSpec(memory_space=pl.ANY) for _ in range(6 + len(every))],
        out_specs=[vmem(), vmem()],
        scratch_shapes=[
            *[pltpu.VMEM(t.shape, t.dtype) for t in given if t is not previous],
            pltpu.VMEM((half, waves), BF16),
            pltpu.VMEM((2 * sticks, waves), BF16),
            pltpu.VMEM((parts, 16, waves), BF16),
            pltpu.VMEM((depth, owners * parts, sticks), F32),
            message,
            message,
            message,
            message,
            pltpu.VMEM((owners, 1, sticks), jnp.int32),
            pltpu.VMEM((groups, 256, 4 * sticks), BF16),
            pltpu.VMEM((groups, 4 * sticks, 256), BF16),
            pltpu.VMEM((groups, 16, 4 * sticks), BF16),
            pltpu.VMEM((groups, parts, 4 * sticks), F32),
            pltpu.VMEM((bands, groups * 16, 256), BF16),
            pltpu.VMEM((bands, groups * 16, 256), BF16),
            pltpu.VMEM((parts, groups * 16, 256), BF16),
            pltpu.VMEM((depth, grid, 256), F32),
            pltpu.VMEM((2, grid, 128), F32),
            pltpu.VMEM((2 * subs, waves), BF16),
            pltpu.VMEM((256, 128), BF16),
            pltpu.VMEM((teams, *previous.shape), BF16),
            sums,
            sums,
            pltpu.VMEM((owners, 2, 128), F32),
            pltpu.SemaphoreType.DMA((17,)),
            one, four, several, four, several, several, several, one, one, one, one, one, one,
        ],
        compiler_params=pltpu.CompilerParams(
            vmem_limit_bytes=60 * 2**20, collective_id=0, has_side_effects=True
        ),
        name="apply",
    )(*given))


def solution(mesh):
    return jax.shard_map(
        per_device,
        mesh=mesh,
        in_specs=(
            P("band", None, "fft"),
            P("fft"),
            P("fft"),
            P("fft", None, None),
            P("band", None, "fft"),
            P("band", None, "fft"),
        ),
        out_specs=(P("band", None, "fft"), P(None, "fft", "band")),
        check_vma=False,
    )
```

```python
import functools
import math

import jax
import jax.numpy as jnp
import numpy as np
from jax import lax
from jax.experimental import pallas as pl
from jax.experimental.pallas import tpu as pltpu
from jax.sharding import PartitionSpec as P

F32 = jnp.float32
BF16 = jnp.bfloat16
NT = (((1,), (1,)), ((), ()))


def dot(a, b):
    return jnp.dot(a, b, preferred_element_type=F32)


def dot_nt(a, b):
    return lax.dot_general(a, b, NT, preferred_element_type=F32)


def tables(grid, owners):
    depth = grid // owners
    block = 4 * depth
    half = grid // 2
    lanes = 128
    k = np.arange(grid)
    m = np.arange(half)
    zorder = (k % owners) * depth + k // owners

    def bf16(t):
        return jnp.asarray(t, BF16)

    def waves(rows, cols, sign, scale):
        angle = 2.0 * math.pi * ((rows[:, None] * cols[None, :]) % grid) / grid
        return np.cos(angle) * scale, sign * np.sin(angle) * scale

    def joined(c, s, rows, cols, height, width):
        out = np.zeros((2 * height, 2 * width))
        out[np.ix_(rows, cols)] = c
        out[np.ix_(height + rows, cols)] = -s
        out[np.ix_(rows, width + cols)] = s
        out[np.ix_(height + rows, width + cols)] = c
        return out

    xpos = 16 * (m // block) + m % block
    wide = groups16(owners) // 2
    order = np.concatenate([k[0::2], k[1::2]])
    zf = waves(zorder, order, 1.0, 1.0)
    zb = waves(order, zorder, -1.0, 1.0 / grid)
    made = [np.concatenate([zf[0], -zf[1]], 1), np.concatenate([zf[1], zf[0]], 1)]
    made += [np.concatenate([zb[0], -zb[1]], 1), np.concatenate([zb[1], zb[0]], 1)]
    for odd in range(2):
        made.append(joined(*waves(m, 2 * m + odd, 1.0, 1.0), m, m, lanes, lanes))
    for odd in range(2):
        made.append(joined(*waves(m, 2 * m + odd, 1.0, 1.0), xpos, m, wide, half).T)
    for odd in range(2):
        made.append(joined(*waves(2 * m + odd, m, -1.0, 1.0 / grid), m, xpos, half, wide).T)
    for odd in range(2):
        made.append(joined(*waves(2 * m + odd, m, -1.0, 1.0 / grid), m, m, lanes, lanes))
    return [bf16(t) for t in made]


def groups16(owners):
    return owners // 4 * 16


def vmem():
    return pl.BlockSpec(memory_space=pltpu.VMEM)


def hot(count, index, numbers):
    lanes = index.shape[1]
    index = jnp.broadcast_to(index.astype(F32), (16, lanes)).astype(BF16)
    rows = numbers[:count].reshape(count // 16, 16, numbers.shape[1])
    rows = jnp.concatenate([rows] * (lanes // numbers.shape[1]), axis=2)
    one, zero = jnp.ones((), BF16), jnp.zeros((), BF16)
    return jnp.where(rows == index[None], one, zero).reshape(count, lanes)


def frequency(values, grid):
    return jnp.where(values >= grid // 2, values - grid, values).astype(F32)


def start_to(src, dst, send_sem, recv_sem, axis, peer):
    pltpu.make_async_remote_copy(
        src_ref=src,
        dst_ref=dst,
        send_sem=send_sem,
        recv_sem=recv_sem,
        device_id={axis: peer},
        device_id_type=pl.DeviceIdType.MESH,
    ).start()


def wait_bytes(ref, sem):
    pltpu.make_async_copy(ref, ref, sem).wait()


def hops(step):
    across, along, over = step
    return min(across, 4 - across) + min(along, 8 - along) + 2 * over


def peers_of(me):
    steps = [(i, j, k) for i in range(4) for j in range(8) for k in range(2)]
    steps = sorted(steps[1:], key=hops, reverse=True)
    across = [16 * lax.rem(lax.div(me, 16) + i, 4) for i in range(4)]
    along = [2 * lax.rem(lax.div(me, 2) + j, 8) for j in range(8)]
    over = [lax.rem(me + k, 2) for k in range(2)]
    return [across[i] + along[j] + over[k] for i, j, k in steps]


def mates_of(team, teams):
    return [lax.rem(team + j, teams) for j in range(1, teams)]


def near(step):
    return lax.rem(lax.div(step * (step + 1), 2), 4)


def kernel(dims, *refs):
    owners, groups, grid, depth, sticks, waves, bands, teams, subs = dims
    inputs, (out, inter), refs = refs[:18], refs[18:20], refs[20:]
    prev = inputs[5]
    held, refs = refs[:17], refs[17:]
    orb, slot, column, pot, sub = held[:5]
    zf, zb, yf, xf, xb, yb = (held[5 + 2 * i : 7 + 2 * i] for i in range(6))
    (high_hot, low_hot, rep, stage, send, recv, send2, recv2, cols, ymask, ymask_t, xmask,
     val, gre, gim, back, pots, turn, left, numbers, pall, r1, r2, r3) = refs[:24]
    (in_s, col_s, col_r, fwd_s, first_r, fwd_r, bwd_s, bwd_r, prev_s, prev_r,
     one_s, one_r, two_s, two_r) = refs[24:]
    parts = 2 * bands
    wide = 4 * sticks
    half = grid // 2
    low = 2 * sticks
    rows = groups * 16
    mid = rows // 2
    chunk = 512
    me = lax.axis_index("fft")
    team = lax.axis_index("band")
    batch = lax.div(lax.rem(me, 16), 4)
    within = 4 * lax.div(me, 16) + lax.rem(me, 4)
    place = 16 * batch + within

    peers, mates = peers_of(me), mates_of(team, teams)

    barrier = pltpu.get_barrier_semaphore()

    def greet(axis, peer):
        pl.semaphore_signal(
            barrier, inc=1, device_id={axis: peer}, device_id_type=pl.DeviceIdType.MESH
        )

    given = [*inputs[:5], *inputs[6:]]
    fetches = [
        pltpu.make_async_copy(src, dst, in_s.at[i])
        for i, (src, dst) in enumerate(zip(given, held, strict=True))
    ]
    for peer in peers:
        greet("fft", peer)
    for i in (1, 0, 2, 5, 6):
        fetches[i].start()
    for mate in mates:
        greet("band", mate)
    for i in (3, 4, *range(7, 17)):
        fetches[i].start()

    with jax.named_scope("hots"):
        numbers[...] = lax.broadcasted_iota(jnp.int32, (256, 128), 0).astype(F32).astype(BF16)
        for i in (0, 1, 2):
            fetches[i].wait()
        for c in range(0, waves, chunk):
            cut = slice(c, c + chunk)
            sl = slot[:, cut]
            high_hot[:, cut] = hot(half, lax.div(sl, low), numbers[...])
            low_hot[:, cut] = hot(low, lax.rem(sl, low), numbers[...])
            for b in range(bands):
                pair = orb[b, :, cut].astype(F32)
                for p in range(2):
                    rep[2 * b + p, :, cut] = jnp.broadcast_to(pair[p : p + 1], (16, chunk)).astype(BF16)

    with jax.named_scope("zdft"):
        got = None
        for c in range(0, waves, chunk):
            cut = slice(c, c + chunk)
            high = high_hot[:, cut].reshape(half // 16, 16, chunk)
            block = jnp.concatenate(
                [(high * rep[r, :, cut][None]).reshape(half, chunk) for r in range(parts)], axis=0
            )
            piece = dot_nt(block, low_hot[:, cut])
            got = piece if got is None else got + piece
        got = got.astype(BF16)
        for i in (5, 6):
            fetches[i].wait()
        for b in range(bands):
            cut = got[2 * b * half : 2 * (b + 1) * half]
            field = jnp.concatenate(
                [cut[p * half : (p + 1) * half, q * sticks : (q + 1) * sticks]
                 for p in range(2) for q in range(2)], axis=0
            )
            for p in range(2):
                done = dot(zf[p][...], field)
                for z in range(depth):
                    at = pl.ds(p * bands + b, owners, stride=parts)
                    stage[z, at, :] = done[z * owners : (z + 1) * owners]
        for z in range(depth):
            for f in range(owners):
                send[z, f] = stage[z, parts * f : parts * (f + 1), :].astype(BF16)

    with jax.named_scope("barrier"):
        pl.semaphore_wait(barrier, owners + teams - 2)
    with jax.named_scope("sends"):
        for peer in peers:
            start_to(column, cols.at[place], col_s, col_r.at[batch], "fft", peer)
        pltpu.make_async_copy(column, cols.at[place], col_r.at[batch]).start()
        for peer in peers:
            start_to(send.at[0, peer], recv.at[0, place], fwd_s.at[0], first_r.at[batch], "fft", peer)
        pltpu.make_async_copy(send.at[0, me], recv.at[0, place], first_r.at[batch]).start()
        for mate in mates:
            start_to(prev, pall.at[team], prev_s, prev_r, "band", mate)
        pltpu.make_async_copy(prev, pall.at[team], prev_r).start()
        for z in range(1, depth):
            for peer in peers:
                start_to(send.at[z, peer], recv.at[z, place], fwd_s.at[z], fwd_r.at[z], "fft", peer)
            pltpu.make_async_copy(send.at[z, me], recv.at[z, place], fwd_r.at[z]).start()

    with jax.named_scope("early"):
        for i in (3, 4, *range(7, 17)):
            fetches[i].wait()
        side = jnp.zeros((grid, 256 - grid), F32)
        gap = jnp.zeros((128 - half, 256), F32)

        def sorted_rows(table):
            for q in range(2):
                turn[q] = table[:, 128 * q : 128 * (q + 1)]
            return [
                jnp.concatenate([turn[q, pl.ds(odd, half, stride=2), :] for q in range(2)], axis=1)
                for odd in range(2)
            ]

        for z in range(depth):
            even, odd = sorted_rows(jnp.concatenate([pot[z], side], axis=1))
            table = jnp.concatenate([even, odd], axis=0).T[:grid]
            even, odd = sorted_rows(jnp.concatenate([table, side], axis=1))
            pots[z] = jnp.concatenate([even, gap, odd, gap], axis=0).T[:grid]
        left[...] = jnp.concatenate([sub[j] for j in range(subs)], axis=0)

    def masks(h):
        g = 4 * lax.rem(h, 4) + lax.div(h, 4)
        for d in range(4):
            col = cols[4 * h + d]
            x = lax.div(col, grid)
            y = col - x * grid
            x = x - 4 * depth * g
            y = jnp.where(y >= half, y + (128 - half), y)
            lanes = slice(sticks * d, sticks * (d + 1))
            ymask[h, :, lanes] = hot(256, y, numbers[...])
            xmask[h, :, lanes] = hot(16, x, numbers[...])
            yt = jnp.broadcast_to(y.astype(F32), (sticks, sticks)).T.astype(BF16)
            line = lax.broadcasted_iota(jnp.int32, (16, 128), 1).astype(F32)
            one, zero = jnp.ones((), BF16), jnp.zeros((), BF16)
            for q in range(2):
                at = (line + 128.0 * q).astype(BF16)[None]
                same = yt.reshape(sticks // 16, 16, 128) == at
                ymask_t[h, lanes, 128 * q : 128 * (q + 1)] = jnp.where(same, one, zero).reshape(sticks, 128)

    def scatter(z, h):
        for d in range(4):
            val[h, :, sticks * d : sticks * (d + 1)] = recv[z, 4 * h + d].astype(F32)
        mask = xmask[h]
        block = jnp.concatenate(
            [mask * jnp.broadcast_to(val[h, r : r + 1, :], (16, wide)).astype(BF16)
             for r in range(parts)], axis=0
        )
        got = dot(block, ymask_t[h]).astype(BF16)
        g = 4 * lax.rem(h, 4) + lax.div(h, 4)
        at = pl.ds(pl.multiple_of(16 * g, 16), 16)
        gre[:, at, :] = got[: bands * 16].reshape(bands, 16, 256)
        gim[:, at, :] = got[bands * 16 :].reshape(bands, 16, 256)

    def local(z):
        ve, vo = pots[z, :half], pots[z, half:]
        every = range(bands)
        ys = []
        for b in every:
            re, im = gre[b], gim[b]
            a = jnp.concatenate([re[:, :128], im[:, :128]], axis=1)
            c = jnp.concatenate([re[:, 128:], im[:, 128:]], axis=1)
            ys.append((dot(a + c, yf[0][...]).astype(BF16), dot(a - c, yf[1][...]).astype(BF16)))
        xs = []
        for b in every:
            e, o = ys[b]
            re = jnp.concatenate([e[:, :128], o[:, :128]], axis=1)
            im = jnp.concatenate([e[:, 128:], o[:, 128:]], axis=1)
            a = jnp.concatenate([re[:mid], im[:mid]], axis=0)
            c = jnp.concatenate([re[mid:], im[mid:]], axis=0)
            we = (dot(xf[0][...], a + c) * jnp.concatenate([ve, ve], axis=0)).astype(BF16)
            wo = (dot(xf[1][...], a - c) * jnp.concatenate([vo, vo], axis=0)).astype(BF16)
            xs.append((we, wo))
        bs = []
        for b in every:
            e = dot(xb[0][...], xs[b][0])
            o = dot(xb[1][...], xs[b][1])
            bs.append(((e + o).astype(BF16), (e - o).astype(BF16)))
        for b in every:
            p, m = bs[b]
            re = jnp.concatenate([p[:mid], m[:mid]], axis=0)
            im = jnp.concatenate([p[mid:], m[mid:]], axis=0)
            e = dot(jnp.concatenate([re[:, :128], im[:, :128]], axis=1), yb[0][...])
            o = dot(jnp.concatenate([re[:, 128:], im[:, 128:]], axis=1), yb[1][...])
            p, m = (e + o).astype(BF16), (e - o).astype(BF16)
            back[b] = jnp.concatenate([p[:, :128], m[:, :128]], axis=1)
            back[bands + b] = jnp.concatenate([p[:, 128:], m[:, 128:]], axis=1)

    around = [lax.rem(batch + o, 4) for o in range(4)]
    across = [lax.rem(lax.div(me, 16) + o, 4) for o in range(4)]
    inside = [lax.rem(lax.rem(me, 4) + o, 4) for o in range(4)]

    def section(z, turns):
        line = lax.broadcasted_iota(jnp.int32, (16, parts * 16), 1)
        row = lax.broadcasted_iota(jnp.int32, (16, parts * 16), 0)
        ones = (lax.div(line, 16) == row).astype(F32).astype(BF16)
        spots = [(4 * around[o] + k, 4 * k + around[o]) for o in turns for k in range(4)]
        tall = []
        for h, g in spots:
            at = pl.ds(pl.multiple_of(16 * g, 16), 16)
            tall.append(dot(back[:, at, :].reshape(parts * 16, 256), ymask[h]))
        cut = []
        for t, (h, g) in zip(tall, spots, strict=True):
            t = t.astype(BF16).reshape(parts, 16, wide) * xmask[h][None]
            cut.append(t.reshape(parts * 16, wide))
        for t, (h, g) in zip(cut, spots, strict=True):
            got = dot(ones, t)[:parts]
            for d in range(4):
                send2[z, 4 * h + d] = got[:, sticks * d : sticks * (d + 1)].astype(BF16)
        for o in turns:
            for y in (2, 1, 3, 0):
                for r in (2, 1, 3, 0):
                    spot = 16 * around[o] + 4 * across[y] + inside[r]
                    peer = 16 * across[y] + 4 * around[o] + inside[r]
                    if o or y or r:
                        start_to(send2.at[z, spot], recv2.at[z, me], bwd_s.at[z], bwd_r.at[z], "fft", peer)
                    else:
                        pltpu.make_async_copy(send2.at[z, spot], recv2.at[z, me], bwd_r.at[z]).start()

    def work(z):
        with jax.named_scope("local"):
            local(z)

        with jax.named_scope("pick"):
            section(z, (2, 3))
            section(z, (1, 0))

    def overlaps():
        wait_bytes(pall, prev_r)
        for t in range(teams):
            right = jnp.concatenate(
                [pall[t, i][p : p + 1] for p in range(2) for i in range(bands)], axis=0
            )
            part = dot_nt(left[...], right)
            part = jnp.concatenate(
                [part, jnp.zeros((2 * subs, 128 - parts), F32)], axis=1
            )
            for j in range(subs):
                r1[t, j] = part[2 * j : 2 * j + 2, :]
        for mate in mates:
            start_to(r1.at[mate], r2.at[team], one_s, one_r, "band", mate)
        pltpu.make_async_copy(r1.at[team], r2.at[team], one_r).start()

    def first(i, carry):
        @pl.when(i == 3)
        def _():
            overlaps()

        q = lax.rem(batch + near(i), 4)
        wait_bytes(cols.at[pl.ds(16 * q, 16)], col_r.at[q])
        for k in range(4):
            masks(4 * q + k)
        wait_bytes(recv.at[0, pl.ds(16 * q, 16)], first_r.at[q])
        for k in range(4):
            scatter(0, 4 * q + k)
        return carry

    with jax.named_scope("first"):
        lax.fori_loop(0, 4, first, 0)

    def plane(z, carry):
        @pl.when(z > 0)
        def _():
            wait_bytes(recv.at[z], fwd_r.at[z])

            def step(h, carry):
                scatter(z, h)
                return carry

            with jax.named_scope("scatter"):
                lax.fori_loop(0, groups, step, 0, unroll=8)

        work(z)

        return carry

    lax.fori_loop(0, depth, plane, 0)

    with jax.named_scope("inter2"):
        wait_bytes(r2, one_r)
        for peer in peers:
            start_to(
                r2.at[lax.div(peer, subs), lax.rem(peer, subs)], r3.at[me], two_s, two_r, "fft", peer
            )
        pltpu.make_async_copy(
            r2.at[lax.div(me, subs), lax.rem(me, subs)], r3.at[me], two_r).start()

    with jax.named_scope("waitback"):
        col = column[...]
        x = lax.div(col, grid)
        y = col - x * grid
        coords = jnp.concatenate([x, y, x, y, x, y, x, y], axis=0).astype(F32).astype(BF16)
        coords = jnp.concatenate([coords, coords], axis=1)
        for z in range(depth):
            wait_bytes(recv2.at[z], bwd_r.at[z])
            for f in range(owners):
                stage[z, parts * f : parts * (f + 1), :] = recv2[z, f].astype(F32)
    with jax.named_scope("zback"):
        lines = []
        for b in range(bands):
            field = jnp.concatenate(
                [stage[z, pl.ds(p * bands + b, owners, stride=parts), :].astype(BF16)
                 for p in range(2) for z in range(depth)], axis=0
            )
            for p in range(2):
                done = dot(zb[p][...], field).astype(BF16)
                lines.append(jnp.concatenate([done[:half], done[half:]], axis=1))
        lines = jnp.concatenate(lines, axis=0)
    with jax.named_scope("pickw"):
        for c in range(0, waves, chunk):
            cut = slice(c, c + chunk)
            plane_at = lax.div(slot[:, cut], sticks)
            low_cut = low_hot[:, cut]
            xy = dot(coords, low_cut)
            fz = frequency(plane_at, grid)
            fx = frequency(xy[0:1].astype(jnp.int32), grid)
            fy = frequency(xy[1:2].astype(jnp.int32), grid)
            kinetic = (fz * fz + fx * fx + fy * fy) * (2.0 / (grid * grid))
            t = dot(lines, low_cut).reshape(parts, half, chunk)
            got = jnp.sum(t * high_hot[:, cut].astype(F32)[None], axis=1)
            for b in range(bands):
                out[b, :, cut] = (
                    got[2 * b : 2 * b + 2] + kinetic * orb[b, :, cut].astype(F32)
                ).astype(BF16)

    with jax.named_scope("waits"):
        wait_bytes(r3, two_r)
        total = jnp.sum(r3[...], axis=0)
        moved = pltpu.roll(total, 128 - bands, 1)
        inter[0] = (total[0:1] + moved[1:2])[:, :bands]
        inter[1] = (moved[0:1] - total[1:2])[:, :bands]
        rest = pl.ds(0, owners - 1)
        for z in range(depth):
            wait_bytes(send.at[z, rest], fwd_s.at[z])
            wait_bytes(send2.at[z, rest], bwd_s.at[z])
        wait_bytes(cols.at[rest], col_s)
        wait_bytes(r3.at[rest], two_s)
        wait_bytes(pall.at[pl.ds(0, teams - 1)], prev_s)
        wait_bytes(r1.at[pl.ds(0, teams - 1)], one_s)


def per_device(orbitals, sphere_slot, stick_column, potential, subspace, previous):
    owners = lax.axis_size("fft")
    teams = lax.axis_size("band")
    groups = owners // 4
    depth, grid, _ = potential.shape
    sticks = stick_column.shape[0]
    waves = sphere_slot.shape[0]
    bands = orbitals.shape[0]
    subs = subspace.shape[0]
    parts = 2 * bands
    half = grid // 2
    every = tables(grid, owners)
    given = [
        orbitals,
        sphere_slot.reshape(1, waves),
        stick_column.reshape(1, sticks),
        potential,
        subspace,
        previous,
        *every,
    ]
    dims = (owners, groups, grid, depth, sticks, waves, bands, teams, subs)
    message = pltpu.VMEM((depth, owners, parts, sticks), BF16)
    sums = pltpu.VMEM((teams, subs, 2, 128), F32)
    one = pltpu.SemaphoreType.DMA
    four = pltpu.SemaphoreType.DMA((4,))
    several = pltpu.SemaphoreType.DMA((depth,))
    return tuple(pl.pallas_call(
        functools.partial(kernel, dims),
        out_shape=[
            jax.ShapeDtypeStruct(orbitals.shape, BF16),
            jax.ShapeDtypeStruct((2, 1, bands), F32),
        ],
        in_specs=[pl.BlockSpec(memory_space=pl.ANY) for _ in range(6 + len(every))],
        out_specs=[vmem(), vmem()],
        scratch_shapes=[
            *[pltpu.VMEM(t.shape, t.dtype) for t in given if t is not previous],
            pltpu.VMEM((half, waves), BF16),
            pltpu.VMEM((2 * sticks, waves), BF16),
            pltpu.VMEM((parts, 16, waves), BF16),
            pltpu.VMEM((depth, owners * parts, sticks), F32),
            message,
            message,
            message,
            message,
            pltpu.VMEM((owners, 1, sticks), jnp.int32),
            pltpu.VMEM((groups, 256, 4 * sticks), BF16),
            pltpu.VMEM((groups, 4 * sticks, 256), BF16),
            pltpu.VMEM((groups, 16, 4 * sticks), BF16),
            pltpu.VMEM((groups, parts, 4 * sticks), F32),
            pltpu.VMEM((bands, groups * 16, 256), BF16),
            pltpu.VMEM((bands, groups * 16, 256), BF16),
            pltpu.VMEM((parts, groups * 16, 256), BF16),
            pltpu.VMEM((depth, grid, 256), F32),
            pltpu.VMEM((2, grid, 128), F32),
            pltpu.VMEM((2 * subs, waves), BF16),
            pltpu.VMEM((256, 128), BF16),
            pltpu.VMEM((teams, *previous.shape), BF16),
            sums,
            sums,
            pltpu.VMEM((owners, 2, 128), F32),
            pltpu.SemaphoreType.DMA((17,)),
            one, four, several, four, several, several, several, one, one, one, one, one, one,
        ],
        compiler_params=pltpu.CompilerParams(
            vmem_limit_bytes=60 * 2**20, collective_id=0, has_side_effects=True
        ),
        name="apply",
    )(*given))


def solution(mesh):
    return jax.shard_map(
        per_device,
        mesh=mesh,
        in_specs=(
            P("band", None, "fft"),
            P("fft"),
            P("fft"),
            P("fft", None, None),
            P("band", None, "fft"),
            P("band", None, "fft"),
        ),
        out_specs=(P("band", None, "fft"), P(None, "fft", "band")),
        check_vma=False,
    )
```

```python
import functools
import math

import jax
import jax.numpy as jnp
import numpy as np
from jax import lax
from jax.experimental import pallas as pl
from jax.experimental.pallas import tpu as pltpu
from jax.sharding import PartitionSpec as P

F32 = jnp.float32
BF16 = jnp.bfloat16
NT = (((1,), (1,)), ((), ()))


def dot(a, b):
    return jnp.dot(a, b, preferred_element_type=F32)


def dot_nt(a, b):
    return lax.dot_general(a, b, NT, preferred_element_type=F32)


def tables(grid, owners):
    depth = grid // owners
    block = 4 * depth
    half = grid // 2
    lanes = 128
    k = np.arange(grid)
    m = np.arange(half)
    zorder = (k % owners) * depth + k // owners

    def bf16(t):
        return jnp.asarray(t, BF16)

    def waves(rows, cols, sign, scale):
        angle = 2.0 * math.pi * ((rows[:, None] * cols[None, :]) % grid) / grid
        return np.cos(angle) * scale, sign * np.sin(angle) * scale

    def joined(c, s, rows, cols, height, width):
        out = np.zeros((2 * height, 2 * width))
        out[np.ix_(rows, cols)] = c
        out[np.ix_(height + rows, cols)] = -s
        out[np.ix_(rows, width + cols)] = s
        out[np.ix_(height + rows, width + cols)] = c
        return out

    xpos = 16 * (m // block) + m % block
    wide = groups16(owners) // 2
    order = np.concatenate([k[0::2], k[1::2]])
    zf = waves(zorder, order, 1.0, 1.0)
    zb = waves(order, zorder, -1.0, 1.0 / grid)
    made = [np.concatenate([zf[0], -zf[1]], 1), np.concatenate([zf[1], zf[0]], 1)]
    made += [np.concatenate([zb[0], -zb[1]], 1), np.concatenate([zb[1], zb[0]], 1)]
    for odd in range(2):
        made.append(joined(*waves(m, 2 * m + odd, 1.0, 1.0), m, m, lanes, lanes))
    for odd in range(2):
        made.append(joined(*waves(m, 2 * m + odd, 1.0, 1.0), xpos, m, wide, half).T)
    for odd in range(2):
        made.append(joined(*waves(2 * m + odd, m, -1.0, 1.0 / grid), m, xpos, half, wide).T)
    for odd in range(2):
        made.append(joined(*waves(2 * m + odd, m, -1.0, 1.0 / grid), m, m, lanes, lanes))
    return [bf16(t) for t in made]


def groups16(owners):
    return owners // 4 * 16


def vmem():
    return pl.BlockSpec(memory_space=pltpu.VMEM)


def hot(count, index, numbers):
    lanes = index.shape[1]
    index = jnp.broadcast_to(index.astype(F32), (16, lanes)).astype(BF16)
    rows = numbers[:count].reshape(count // 16, 16, numbers.shape[1])
    rows = jnp.concatenate([rows] * (lanes // numbers.shape[1]), axis=2)
    one, zero = jnp.ones((), BF16), jnp.zeros((), BF16)
    return jnp.where(rows == index[None], one, zero).reshape(count, lanes)


def frequency(values, grid):
    return jnp.where(values >= grid // 2, values - grid, values).astype(F32)


def start_to(src, dst, send_sem, recv_sem, axis, peer):
    pltpu.make_async_remote_copy(
        src_ref=src,
        dst_ref=dst,
        send_sem=send_sem,
        recv_sem=recv_sem,
        device_id={axis: peer},
        device_id_type=pl.DeviceIdType.MESH,
    ).start()


def wait_bytes(ref, sem):
    pltpu.make_async_copy(ref, ref, sem).wait()


def hops(step):
    across, along, over = step
    return min(across, 4 - across) + min(along, 8 - along) + 2 * over


def peers_of(me):
    steps = [(i, j, k) for i in range(4) for j in range(8) for k in range(2)]
    steps = sorted(steps[1:], key=hops, reverse=True)
    across = [16 * lax.rem(lax.div(me, 16) + i, 4) for i in range(4)]
    along = [2 * lax.rem(lax.div(me, 2) + j, 8) for j in range(8)]
    over = [lax.rem(me + k, 2) for k in range(2)]
    return [across[i] + along[j] + over[k] for i, j, k in steps]


def mates_of(team, teams):
    return [lax.rem(team + j, teams) for j in range(1, teams)]


def near(step):
    return lax.rem(lax.div(step * (step + 1), 2), 4)


def kernel(dims, *refs):
    owners, groups, grid, depth, sticks, waves, bands, teams, subs = dims
    half, rows, wide = grid // 2, groups * 16, 4 * sticks
    shapes = [
        (half, waves), (2 * sticks, waves), (2 * bands, 16, waves),
        (groups, 256, wide), (groups, wide, 256), (groups, 16, wide),
        (bands, rows, 256), (bands, rows, 256), (2 * bands, rows, 256),
        (2 * subs, waves), (256, 128), *[ref.shape for ref in refs[10:18]],
    ]
    pl.run_scoped(
        functools.partial(apply, dims, refs), *[pltpu.VMEM(shape, BF16) for shape in shapes]
    )


def apply(dims, refs, *near_refs):
    owners, groups, grid, depth, sticks, waves, bands, teams, subs = dims
    inputs, (out, inter), refs = refs[:18], refs[18:20], refs[20:]
    prev = inputs[5]
    held, refs = refs[:17], refs[17:]
    orb, slot, column, pot, sub = held[:5]
    zf, zb = held[5:7], held[7:9]
    (high_hot, low_hot, rep, ymask, ymask_t, xmask, gre, gim, back, left, numbers) = near_refs[:11]
    fixed = near_refs[11:]
    yf, xf, xb, yb = (fixed[2 * i : 2 * i + 2] for i in range(4))
    (stage, send, recv, send2, recv2, cols, val, pots, turn, pall, r1, r2, r3) = refs[:13]
    (in_s, col_s, col_r, fwd_s, first_r, fwd_r, bwd_s, bwd_r, prev_s, prev_r,
     one_s, one_r, two_s, two_r) = refs[13:]
    parts = 2 * bands
    wide = 4 * sticks
    half = grid // 2
    low = 2 * sticks
    rows = groups * 16
    mid = rows // 2
    chunk = 512
    me = lax.axis_index("fft")
    team = lax.axis_index("band")
    batch = lax.div(lax.rem(me, 16), 4)
    within = 4 * lax.div(me, 16) + lax.rem(me, 4)
    place = 16 * batch + within

    peers, mates = peers_of(me), mates_of(team, teams)

    barrier = pltpu.get_barrier_semaphore()

    def greet(axis, peer):
        pl.semaphore_signal(
            barrier, inc=1, device_id={axis: peer}, device_id_type=pl.DeviceIdType.MESH
        )

    given = [*inputs[:5], *inputs[6:]]
    fetches = [
        pltpu.make_async_copy(src, dst, in_s.at[i])
        for i, (src, dst) in enumerate(zip(given, held, strict=True))
    ]
    for peer in peers:
        greet("fft", peer)
    for i in (1, 0, 2, 5, 6):
        fetches[i].start()
    for mate in mates:
        greet("band", mate)
    for i in (3, 4, *range(7, 17)):
        fetches[i].start()

    with jax.named_scope("hots"):
        numbers[...] = lax.broadcasted_iota(jnp.int32, (256, 128), 0).astype(F32).astype(BF16)
        for i in (0, 1, 2):
            fetches[i].wait()
        for c in range(0, waves, chunk):
            cut = slice(c, c + chunk)
            sl = slot[:, cut]
            high_hot[:, cut] = hot(half, lax.div(sl, low), numbers[...])
            low_hot[:, cut] = hot(low, lax.rem(sl, low), numbers[...])
            for b in range(bands):
                pair = orb[b, :, cut].astype(F32)
                for p in range(2):
                    rep[2 * b + p, :, cut] = jnp.broadcast_to(pair[p : p + 1], (16, chunk)).astype(BF16)

    with jax.named_scope("zdft"):
        got = None
        for c in range(0, waves, chunk):
            cut = slice(c, c + chunk)
            high = high_hot[:, cut].reshape(half // 16, 16, chunk)
            block = jnp.concatenate(
                [(high * rep[r, :, cut][None]).reshape(half, chunk) for r in range(parts)], axis=0
            )
            piece = dot_nt(block, low_hot[:, cut])
            got = piece if got is None else got + piece
        got = got.astype(BF16)
        for i in (5, 6):
            fetches[i].wait()
        for b in range(bands):
            cut = got[2 * b * half : 2 * (b + 1) * half]
            field = jnp.concatenate(
                [cut[p * half : (p + 1) * half, q * sticks : (q + 1) * sticks]
                 for p in range(2) for q in range(2)], axis=0
            )
            for p in range(2):
                done = dot(zf[p][...], field)
                for z in range(depth):
                    at = pl.ds(p * bands + b, owners, stride=parts)
                    stage[z, at, :] = done[z * owners : (z + 1) * owners]
        for z in range(depth):
            for f in range(owners):
                send[z, f] = stage[z, parts * f : parts * (f + 1), :].astype(BF16)

    with jax.named_scope("barrier"):
        pl.semaphore_wait(barrier, owners + teams - 2)
    with jax.named_scope("sends"):
        for peer in peers:
            start_to(column, cols.at[place], col_s, col_r.at[batch], "fft", peer)
        pltpu.make_async_copy(column, cols.at[place], col_r.at[batch]).start()
        for peer in peers:
            start_to(send.at[0, peer], recv.at[0, place], fwd_s.at[0], first_r.at[batch], "fft", peer)
        pltpu.make_async_copy(send.at[0, me], recv.at[0, place], first_r.at[batch]).start()
        for mate in mates:
            start_to(prev, pall.at[team], prev_s, prev_r, "band", mate)
        pltpu.make_async_copy(prev, pall.at[team], prev_r).start()
        for z in range(1, depth):
            for peer in peers:
                start_to(send.at[z, peer], recv.at[z, place], fwd_s.at[z], fwd_r.at[z], "fft", peer)
            pltpu.make_async_copy(send.at[z, me], recv.at[z, place], fwd_r.at[z]).start()

    with jax.named_scope("early"):
        for i in (3, 4, *range(7, 17)):
            fetches[i].wait()
        side = jnp.zeros((grid, 256 - grid), F32)
        gap = jnp.zeros((128 - half, 256), F32)

        def sorted_rows(table):
            for q in range(2):
                turn[q] = table[:, 128 * q : 128 * (q + 1)]
            return [
                jnp.concatenate([turn[q, pl.ds(odd, half, stride=2), :] for q in range(2)], axis=1)
                for odd in range(2)
            ]

        for z in range(depth):
            even, odd = sorted_rows(jnp.concatenate([pot[z], side], axis=1))
            table = jnp.concatenate([even, odd], axis=0).T[:grid]
            even, odd = sorted_rows(jnp.concatenate([table, side], axis=1))
            pots[z] = jnp.concatenate([even, gap, odd, gap], axis=0).T[:grid]
        for src, dst in zip(held[9:], fixed, strict=True):
            dst[...] = src[...]
        left[...] = jnp.concatenate([sub[j] for j in range(subs)], axis=0)

    def masks(h):
        g = 4 * lax.rem(h, 4) + lax.div(h, 4)
        for d in range(4):
            col = cols[4 * h + d]
            x = lax.div(col, grid)
            y = col - x * grid
            x = x - 4 * depth * g
            y = jnp.where(y >= half, y + (128 - half), y)
            lanes = slice(sticks * d, sticks * (d + 1))
            ymask[h, :, lanes] = hot(256, y, numbers[...])
            xmask[h, :, lanes] = hot(16, x, numbers[...])
            yt = jnp.broadcast_to(y.astype(F32), (sticks, sticks)).T.astype(BF16)
            line = lax.broadcasted_iota(jnp.int32, (16, 128), 1).astype(F32)
            one, zero = jnp.ones((), BF16), jnp.zeros((), BF16)
            for q in range(2):
                at = (line + 128.0 * q).astype(BF16)[None]
                same = yt.reshape(sticks // 16, 16, 128) == at
                ymask_t[h, lanes, 128 * q : 128 * (q + 1)] = jnp.where(same, one, zero).reshape(sticks, 128)

    def scatter(z, h):
        for d in range(4):
            val[h, :, sticks * d : sticks * (d + 1)] = recv[z, 4 * h + d].astype(F32)
        mask = xmask[h]
        block = jnp.concatenate(
            [mask * jnp.broadcast_to(val[h, r : r + 1, :], (16, wide)).astype(BF16)
             for r in range(parts)], axis=0
        )
        got = dot(block, ymask_t[h]).astype(BF16)
        g = 4 * lax.rem(h, 4) + lax.div(h, 4)
        at = pl.ds(pl.multiple_of(16 * g, 16), 16)
        gre[:, at, :] = got[: bands * 16].reshape(bands, 16, 256)
        gim[:, at, :] = got[bands * 16 :].reshape(bands, 16, 256)

    def local(z):
        ve, vo = pots[z, :half], pots[z, half:]
        every = range(bands)
        ys = []
        for b in every:
            re, im = gre[b], gim[b]
            a = jnp.concatenate([re[:, :128], im[:, :128]], axis=1)
            c = jnp.concatenate([re[:, 128:], im[:, 128:]], axis=1)
            ys.append((dot(a + c, yf[0][...]).astype(BF16), dot(a - c, yf[1][...]).astype(BF16)))
        xs = []
        for b in every:
            e, o = ys[b]
            re = jnp.concatenate([e[:, :128], o[:, :128]], axis=1)
            im = jnp.concatenate([e[:, 128:], o[:, 128:]], axis=1)
            a = jnp.concatenate([re[:mid], im[:mid]], axis=0)
            c = jnp.concatenate([re[mid:], im[mid:]], axis=0)
            we = (dot(xf[0][...], a + c) * jnp.concatenate([ve, ve], axis=0)).astype(BF16)
            wo = (dot(xf[1][...], a - c) * jnp.concatenate([vo, vo], axis=0)).astype(BF16)
            xs.append((we, wo))
        bs = []
        for b in every:
            e = dot(xb[0][...], xs[b][0])
            o = dot(xb[1][...], xs[b][1])
            bs.append(((e + o).astype(BF16), (e - o).astype(BF16)))
        for b in every:
            p, m = bs[b]
            re = jnp.concatenate([p[:mid], m[:mid]], axis=0)
            im = jnp.concatenate([p[mid:], m[mid:]], axis=0)
            e = dot(jnp.concatenate([re[:, :128], im[:, :128]], axis=1), yb[0][...])
            o = dot(jnp.concatenate([re[:, 128:], im[:, 128:]], axis=1), yb[1][...])
            p, m = (e + o).astype(BF16), (e - o).astype(BF16)
            back[b] = jnp.concatenate([p[:, :128], m[:, :128]], axis=1)
            back[bands + b] = jnp.concatenate([p[:, 128:], m[:, 128:]], axis=1)

    around = [lax.rem(batch + o, 4) for o in range(4)]
    across = [lax.rem(lax.div(me, 16) + o, 4) for o in range(4)]
    inside = [lax.rem(lax.rem(me, 4) + o, 4) for o in range(4)]

    def section(z, turns):
        line = lax.broadcasted_iota(jnp.int32, (16, parts * 16), 1)
        row = lax.broadcasted_iota(jnp.int32, (16, parts * 16), 0)
        ones = (lax.div(line, 16) == row).astype(F32).astype(BF16)
        spots = [(4 * around[o] + k, 4 * k + around[o]) for o in turns for k in range(4)]
        tall = []
        for h, g in spots:
            at = pl.ds(pl.multiple_of(16 * g, 16), 16)
            tall.append(dot(back[:, at, :].reshape(parts * 16, 256), ymask[h]))
        cut = []
        for t, (h, g) in zip(tall, spots, strict=True):
            t = t.astype(BF16).reshape(parts, 16, wide) * xmask[h][None]
            cut.append(t.reshape(parts * 16, wide))
        for t, (h, g) in zip(cut, spots, strict=True):
            got = dot(ones, t)[:parts]
            for d in range(4):
                send2[z, 4 * h + d] = got[:, sticks * d : sticks * (d + 1)].astype(BF16)
        for o in turns:
            for y in (2, 1, 3, 0):
                for r in (2, 1, 3, 0):
                    spot = 16 * around[o] + 4 * across[y] + inside[r]
                    peer = 16 * across[y] + 4 * around[o] + inside[r]
                    if o or y or r:
                        start_to(send2.at[z, spot], recv2.at[z, me], bwd_s.at[z], bwd_r.at[z], "fft", peer)
                    else:
                        pltpu.make_async_copy(send2.at[z, spot], recv2.at[z, me], bwd_r.at[z]).start()

    def work(z):
        with jax.named_scope("local"):
            local(z)

        with jax.named_scope("pick"):
            section(z, (2, 3))
            section(z, (1, 0))

    def overlaps():
        wait_bytes(pall, prev_r)
        for t in range(teams):
            right = jnp.concatenate(
                [pall[t, i][p : p + 1] for p in range(2) for i in range(bands)], axis=0
            )
            part = dot_nt(left[...], right)
            part = jnp.concatenate(
                [part, jnp.zeros((2 * subs, 128 - parts), F32)], axis=1
            )
            for j in range(subs):
                r1[t, j] = part[2 * j : 2 * j + 2, :]
        for mate in mates:
            start_to(r1.at[mate], r2.at[team], one_s, one_r, "band", mate)
        pltpu.make_async_copy(r1.at[team], r2.at[team], one_r).start()

    def first(i, carry):
        @pl.when(i == 3)
        def _():
            overlaps()

        q = lax.rem(batch + near(i), 4)
        wait_bytes(cols.at[pl.ds(16 * q, 16)], col_r.at[q])
        for k in range(4):
            masks(4 * q + k)
        wait_bytes(recv.at[0, pl.ds(16 * q, 16)], first_r.at[q])
        for k in range(4):
            scatter(0, 4 * q + k)
        return carry

    with jax.named_scope("first"):
        lax.fori_loop(0, 4, first, 0)

    def plane(z, carry):
        @pl.when(z > 0)
        def _():
            wait_bytes(recv.at[z], fwd_r.at[z])

            def step(h, carry):
                scatter(z, h)
                return carry

            with jax.named_scope("scatter"):
                lax.fori_loop(0, groups, step, 0, unroll=8)

        work(z)

        return carry

    lax.fori_loop(0, depth, plane, 0)

    with jax.named_scope("inter2"):
        wait_bytes(r2, one_r)
        for peer in peers:
            start_to(
                r2.at[lax.div(peer, subs), lax.rem(peer, subs)], r3.at[me], two_s, two_r, "fft", peer
            )
        pltpu.make_async_copy(
            r2.at[lax.div(me, subs), lax.rem(me, subs)], r3.at[me], two_r).start()

    with jax.named_scope("waitback"):
        col = column[...]
        x = lax.div(col, grid)
        y = col - x * grid
        coords = jnp.concatenate([x, y, x, y, x, y, x, y], axis=0).astype(F32).astype(BF16)
        coords = jnp.concatenate([coords, coords], axis=1)
        for z in range(depth):
            wait_bytes(recv2.at[z], bwd_r.at[z])
            for f in range(owners):
                stage[z, parts * f : parts * (f + 1), :] = recv2[z, f].astype(F32)
    with jax.named_scope("zback"):
        lines = []
        for b in range(bands):
            field = jnp.concatenate(
                [stage[z, pl.ds(p * bands + b, owners, stride=parts), :].astype(BF16)
                 for p in range(2) for z in range(depth)], axis=0
            )
            for p in range(2):
                done = dot(zb[p][...], field).astype(BF16)
                lines.append(jnp.concatenate([done[:half], done[half:]], axis=1))
        lines = jnp.concatenate(lines, axis=0)
    with jax.named_scope("pickw"):
        for c in range(0, waves, chunk):
            cut = slice(c, c + chunk)
            plane_at = lax.div(slot[:, cut], sticks)
            low_cut = low_hot[:, cut]
            xy = dot(coords, low_cut)
            fz = frequency(plane_at, grid)
            fx = frequency(xy[0:1].astype(jnp.int32), grid)
            fy = frequency(xy[1:2].astype(jnp.int32), grid)
            kinetic = (fz * fz + fx * fx + fy * fy) * (2.0 / (grid * grid))
            t = dot(lines, low_cut).reshape(parts, half, chunk)
            got = jnp.sum(t * high_hot[:, cut].astype(F32)[None], axis=1)
            for b in range(bands):
                out[b, :, cut] = (
                    got[2 * b : 2 * b + 2] + kinetic * orb[b, :, cut].astype(F32)
                ).astype(BF16)

    with jax.named_scope("waits"):
        wait_bytes(r3, two_r)
        total = jnp.sum(r3[...], axis=0)
        moved = pltpu.roll(total, 128 - bands, 1)
        inter[0] = (total[0:1] + moved[1:2])[:, :bands]
        inter[1] = (moved[0:1] - total[1:2])[:, :bands]
        rest = pl.ds(0, owners - 1)
        for z in range(depth):
            wait_bytes(send.at[z, rest], fwd_s.at[z])
            wait_bytes(send2.at[z, rest], bwd_s.at[z])
        wait_bytes(cols.at[rest], col_s)
        wait_bytes(r3.at[rest], two_s)
        wait_bytes(pall.at[pl.ds(0, teams - 1)], prev_s)
        wait_bytes(r1.at[pl.ds(0, teams - 1)], one_s)


def deliver(applied, inter, out, sums, sems):
    copies = [
        pltpu.make_async_copy(applied, out, sems.at[0]),
        pltpu.make_async_copy(inter, sums, sems.at[1]),
    ]
    for copy in copies:
        copy.start()
    for copy in copies:
        copy.wait()


def per_device(orbitals, sphere_slot, stick_column, potential, subspace, previous):
    owners = lax.axis_size("fft")
    teams = lax.axis_size("band")
    groups = owners // 4
    depth, grid, _ = potential.shape
    sticks = stick_column.shape[0]
    waves = sphere_slot.shape[0]
    bands = orbitals.shape[0]
    subs = subspace.shape[0]
    parts = 2 * bands
    half = grid // 2
    every = tables(grid, owners)
    given = [
        orbitals,
        sphere_slot.reshape(1, waves),
        stick_column.reshape(1, sticks),
        potential,
        subspace,
        previous,
        *every,
    ]
    dims = (owners, groups, grid, depth, sticks, waves, bands, teams, subs)
    message = pltpu.VMEM((depth, owners, parts, sticks), BF16)
    sums = pltpu.VMEM((teams, subs, 2, 128), F32)
    one = pltpu.SemaphoreType.DMA
    four = pltpu.SemaphoreType.DMA((4,))
    several = pltpu.SemaphoreType.DMA((depth,))
    applied, inter = pl.pallas_call(
        functools.partial(kernel, dims),
        out_shape=[
            pltpu.VMEM(orbitals.shape, BF16),
            pltpu.VMEM((2, 1, bands), F32),
        ],
        in_specs=[pl.BlockSpec(memory_space=pl.ANY) for _ in range(6 + len(every))],
        out_specs=[vmem(), vmem()],
        scratch_shapes=[
            *[pltpu.VMEM(t.shape, t.dtype) for t in given if t is not previous],
            pltpu.VMEM((depth, owners * parts, sticks), F32),
            message,
            message,
            message,
            message,
            pltpu.VMEM((owners, 1, sticks), jnp.int32),
            pltpu.VMEM((groups, parts, 4 * sticks), F32),
            pltpu.VMEM((depth, grid, 256), F32),
            pltpu.VMEM((2, grid, 128), F32),
            pltpu.VMEM((teams, *previous.shape), BF16),
            sums,
            sums,
            pltpu.VMEM((owners, 2, 128), F32),
            pltpu.SemaphoreType.DMA((17,)),
            one, four, several, four, several, several, several, one, one, one, one, one, one,
        ],
        compiler_params=pltpu.CompilerParams(
            vmem_limit_bytes=60 * 2**20, collective_id=0, has_side_effects=True
        ),
        name="apply",
    )(*given)
    return tuple(pl.pallas_call(
        deliver,
        out_shape=[
            jax.ShapeDtypeStruct(orbitals.shape, BF16),
            jax.ShapeDtypeStruct((2, 1, bands), F32),
        ],
        in_specs=[vmem(), vmem()],
        out_specs=[pl.BlockSpec(memory_space=pl.ANY)] * 2,
        scratch_shapes=[pltpu.SemaphoreType.DMA((2,))],
        name="deliver",
    )(pltpu.with_memory_space_constraint(applied, pltpu.VMEM), pltpu.with_memory_space_constraint(inter, pltpu.VMEM)))


def solution(mesh):
    return jax.shard_map(
        per_device,
        mesh=mesh,
        in_specs=(
            P("band", None, "fft"),
            P("fft"),
            P("fft"),
            P("fft", None, None),
            P("band", None, "fft"),
            P("band", None, "fft"),
        ),
        out_specs=(P("band", None, "fft"), P(None, "fft", "band")),
        check_vma=False,
    )
```

```python
import functools
import math

import jax
import jax.numpy as jnp
import numpy as np
from jax import lax
from jax.experimental import pallas as pl
from jax.experimental.pallas import tpu as pltpu
from jax.sharding import PartitionSpec as P

F32 = jnp.float32
BF16 = jnp.bfloat16
NT = (((1,), (1,)), ((), ()))


def dot(a, b):
    return jnp.dot(a, b, preferred_element_type=F32)


def dot_nt(a, b):
    return lax.dot_general(a, b, NT, preferred_element_type=F32)


def tables(grid, owners):
    depth = grid // owners
    block = 4 * depth
    half = grid // 2
    lanes = 128
    k = np.arange(grid)
    m = np.arange(half)
    zorder = (k % owners) * depth + k // owners

    def bf16(t):
        return jnp.asarray(t, BF16)

    def waves(rows, cols, sign, scale):
        angle = 2.0 * math.pi * ((rows[:, None] * cols[None, :]) % grid) / grid
        return np.cos(angle) * scale, sign * np.sin(angle) * scale

    def joined(c, s, rows, cols, height, width):
        out = np.zeros((2 * height, 2 * width))
        out[np.ix_(rows, cols)] = c
        out[np.ix_(height + rows, cols)] = -s
        out[np.ix_(rows, width + cols)] = s
        out[np.ix_(height + rows, width + cols)] = c
        return out

    xpos = 16 * (m // block) + m % block
    wide = groups16(owners) // 2
    order = np.concatenate([k[0::2], k[1::2]])
    zf = waves(zorder, order, 1.0, 1.0)
    zb = waves(order, zorder, -1.0, 1.0 / grid)
    made = [np.concatenate([zf[0], -zf[1]], 1), np.concatenate([zf[1], zf[0]], 1)]
    made += [np.concatenate([zb[0], -zb[1]], 1), np.concatenate([zb[1], zb[0]], 1)]
    for odd in range(2):
        made.append(joined(*waves(m, 2 * m + odd, 1.0, 1.0), m, m, lanes, lanes))
    for odd in range(2):
        made.append(joined(*waves(m, 2 * m + odd, 1.0, 1.0), xpos, m, wide, half).T)
    for odd in range(2):
        made.append(joined(*waves(2 * m + odd, m, -1.0, 1.0 / grid), m, xpos, half, wide).T)
    for odd in range(2):
        made.append(joined(*waves(2 * m + odd, m, -1.0, 1.0 / grid), m, m, lanes, lanes))
    last = depth * np.arange(owners) + depth - 1
    made.append(np.concatenate(
        [t for odd in range(2) for t in waves(last, 2 * m + odd, -1.0, 1.0 / grid)], 0
    ))
    return [bf16(t) for t in made]


def groups16(owners):
    return owners // 4 * 16


def vmem():
    return pl.BlockSpec(memory_space=pltpu.VMEM)


def hot(count, index, numbers):
    lanes = index.shape[1]
    index = jnp.broadcast_to(index.astype(F32), (16, lanes)).astype(BF16)
    rows = numbers[:count].reshape(count // 16, 16, numbers.shape[1])
    rows = jnp.concatenate([rows] * (lanes // numbers.shape[1]), axis=2)
    one, zero = jnp.ones((), BF16), jnp.zeros((), BF16)
    return jnp.where(rows == index[None], one, zero).reshape(count, lanes)


def frequency(values, grid):
    return jnp.where(values >= grid // 2, values - grid, values).astype(F32)


def start_to(src, dst, send_sem, recv_sem, axis, peer):
    pltpu.make_async_remote_copy(
        src_ref=src,
        dst_ref=dst,
        send_sem=send_sem,
        recv_sem=recv_sem,
        device_id={axis: peer},
        device_id_type=pl.DeviceIdType.MESH,
    ).start()


def wait_bytes(ref, sem):
    pltpu.make_async_copy(ref, ref, sem).wait()


def hops(step):
    across, along, over = step
    return min(across, 4 - across) + min(along, 8 - along) + 2 * over


def peers_of(me):
    steps = [(i, j, k) for i in range(4) for j in range(8) for k in range(2)]
    steps = sorted(steps[1:], key=hops, reverse=True)
    across = [16 * lax.rem(lax.div(me, 16) + i, 4) for i in range(4)]
    along = [2 * lax.rem(lax.div(me, 2) + j, 8) for j in range(8)]
    over = [lax.rem(me + k, 2) for k in range(2)]
    return [across[i] + along[j] + over[k] for i, j, k in steps]


def mates_of(team, teams):
    return [lax.rem(team + j, teams) for j in range(1, teams)]


def near(step):
    return lax.rem(lax.div(step * (step + 1), 2), 4)


def kernel(dims, *refs):
    owners, groups, grid, depth, sticks, waves, bands, teams, subs = dims
    half, rows, wide = grid // 2, groups * 16, 4 * sticks
    shapes = [
        (half, waves), (2 * sticks, waves), (2 * bands, 16, waves),
        (groups, 256, wide), (groups, wide, 256), (groups, 16, wide),
        (bands, rows, 256), (bands, rows, 256), (2 * bands, rows, 256),
        (2 * subs, waves), (256, 128), (sticks, waves), *[ref.shape for ref in refs[10:18]],
    ]
    pl.run_scoped(
        functools.partial(apply, dims, refs), *[pltpu.VMEM(shape, BF16) for shape in shapes]
    )


def apply(dims, refs, *near_refs):
    owners, groups, grid, depth, sticks, waves, bands, teams, subs = dims
    inputs, (out, inter), refs = refs[:19], refs[19:21], refs[21:]
    prev = inputs[5]
    held, refs = refs[:18], refs[18:]
    orb, slot, column, pot, sub = held[:5]
    zf, zb = held[5:7], held[7:9]
    (high_hot, low_hot, rep, ymask, ymask_t, xmask, gre, gim, back, left, numbers, shot) = near_refs[:12]
    fixed = near_refs[12:]
    yf, xf, xb, yb = (fixed[2 * i : 2 * i + 2] for i in range(4))
    (stage, send, recv, send2, recv2, cols, val, pots, turn, pall, r1, r2, r3, sofar, swing) = refs[:15]
    (in_s, col_s, col_r, fwd_s, first_r, fwd_r, bwd_s, bwd_r, prev_s, prev_r,
     one_s, one_r, two_s, two_r) = refs[15:]
    parts = 2 * bands
    wide = 4 * sticks
    half = grid // 2
    low = 2 * sticks
    rows = groups * 16
    mid = rows // 2
    chunk = 512
    me = lax.axis_index("fft")
    team = lax.axis_index("band")
    batch = lax.div(lax.rem(me, 16), 4)
    within = 4 * lax.div(me, 16) + lax.rem(me, 4)
    place = 16 * batch + within

    peers, mates = peers_of(me), mates_of(team, teams)

    barrier = pltpu.get_barrier_semaphore()

    def greet(axis, peer):
        pl.semaphore_signal(
            barrier, inc=1, device_id={axis: peer}, device_id_type=pl.DeviceIdType.MESH
        )

    given = [*inputs[:5], *inputs[6:]]
    fetches = [
        pltpu.make_async_copy(src, dst, in_s.at[i])
        for i, (src, dst) in enumerate(zip(given, held, strict=True))
    ]
    for peer in peers:
        greet("fft", peer)
    for i in (1, 0, 2, 5, 6):
        fetches[i].start()
    for mate in mates:
        greet("band", mate)
    for i in (3, 4, *range(7, 18)):
        fetches[i].start()

    with jax.named_scope("hots"):
        numbers[...] = lax.broadcasted_iota(jnp.int32, (256, 128), 0).astype(F32).astype(BF16)
        for i in (0, 1, 2):
            fetches[i].wait()
        for c in range(0, waves, chunk):
            cut = slice(c, c + chunk)
            sl = slot[:, cut]
            high_hot[:, cut] = hot(half, lax.div(sl, low), numbers[...])
            low_hot[:, cut] = hot(low, lax.rem(sl, low), numbers[...])
            for b in range(bands):
                pair = orb[b, :, cut].astype(F32)
                for p in range(2):
                    rep[2 * b + p, :, cut] = jnp.broadcast_to(pair[p : p + 1], (16, chunk)).astype(BF16)

    with jax.named_scope("zdft"):
        got = None
        for c in range(0, waves, chunk):
            cut = slice(c, c + chunk)
            high = high_hot[:, cut].reshape(half // 16, 16, chunk)
            block = jnp.concatenate(
                [(high * rep[r, :, cut][None]).reshape(half, chunk) for r in range(parts)], axis=0
            )
            piece = dot_nt(block, low_hot[:, cut])
            got = piece if got is None else got + piece
        got = got.astype(BF16)
        for i in (5, 6):
            fetches[i].wait()
        for b in range(bands):
            cut = got[2 * b * half : 2 * (b + 1) * half]
            field = jnp.concatenate(
                [cut[p * half : (p + 1) * half, q * sticks : (q + 1) * sticks]
                 for p in range(2) for q in range(2)], axis=0
            )
            for p in range(2):
                done = dot(zf[p][...], field)
                for z in range(depth):
                    at = pl.ds(p * bands + b, owners, stride=parts)
                    stage[z, at, :] = done[z * owners : (z + 1) * owners]
        for z in range(depth):
            for f in range(owners):
                send[z, f] = stage[z, parts * f : parts * (f + 1), :].astype(BF16)

    with jax.named_scope("barrier"):
        pl.semaphore_wait(barrier, owners + teams - 2)
    with jax.named_scope("sends"):
        for peer in peers:
            start_to(column, cols.at[place], col_s, col_r.at[batch], "fft", peer)
        pltpu.make_async_copy(column, cols.at[place], col_r.at[batch]).start()
        for peer in peers:
            start_to(send.at[0, peer], recv.at[0, place], fwd_s.at[0], first_r.at[batch], "fft", peer)
        pltpu.make_async_copy(send.at[0, me], recv.at[0, place], first_r.at[batch]).start()
        for z in range(1, depth):
            for peer in peers:
                start_to(send.at[z, peer], recv.at[z, place], fwd_s.at[z], fwd_r.at[z], "fft", peer)
            pltpu.make_async_copy(send.at[z, me], recv.at[z, place], fwd_r.at[z]).start()
        for mate in mates:
            start_to(prev, pall.at[team], prev_s, prev_r, "band", mate)
        pltpu.make_async_copy(prev, pall.at[team], prev_r).start()

    with jax.named_scope("early"):
        for i in (3, 4, *range(7, 18)):
            fetches[i].wait()
        side = jnp.zeros((grid, 256 - grid), F32)
        gap = jnp.zeros((128 - half, 256), F32)

        def sorted_rows(table):
            for q in range(2):
                turn[q] = table[:, 128 * q : 128 * (q + 1)]
            return [
                jnp.concatenate([turn[q, pl.ds(odd, half, stride=2), :] for q in range(2)], axis=1)
                for odd in range(2)
            ]

        for z in range(depth):
            even, odd = sorted_rows(jnp.concatenate([pot[z], side], axis=1))
            table = jnp.concatenate([even, odd], axis=0).T[:grid]
            even, odd = sorted_rows(jnp.concatenate([table, side], axis=1))
            pots[z] = jnp.concatenate([even, gap, odd, gap], axis=0).T[:grid]
        for src, dst in zip(held[9:17], fixed, strict=True):
            dst[...] = src[...]
        left[...] = jnp.concatenate([sub[j] for j in range(subs)], axis=0)

    def masks(h):
        g = 4 * lax.rem(h, 4) + lax.div(h, 4)
        for d in range(4):
            col = cols[4 * h + d]
            x = lax.div(col, grid)
            y = col - x * grid
            x = x - 4 * depth * g
            y = jnp.where(y >= half, y + (128 - half), y)
            lanes = slice(sticks * d, sticks * (d + 1))
            ymask[h, :, lanes] = hot(256, y, numbers[...])
            xmask[h, :, lanes] = hot(16, x, numbers[...])
            yt = jnp.broadcast_to(y.astype(F32), (sticks, sticks)).T.astype(BF16)
            line = lax.broadcasted_iota(jnp.int32, (16, 128), 1).astype(F32)
            one, zero = jnp.ones((), BF16), jnp.zeros((), BF16)
            for q in range(2):
                at = (line + 128.0 * q).astype(BF16)[None]
                same = yt.reshape(sticks // 16, 16, 128) == at
                ymask_t[h, lanes, 128 * q : 128 * (q + 1)] = jnp.where(same, one, zero).reshape(sticks, 128)

    def scatter(z, h):
        for d in range(4):
            val[h, :, sticks * d : sticks * (d + 1)] = recv[z, 4 * h + d].astype(F32)
        mask = xmask[h]
        block = jnp.concatenate(
            [mask * jnp.broadcast_to(val[h, r : r + 1, :], (16, wide)).astype(BF16)
             for r in range(parts)], axis=0
        )
        got = dot(block, ymask_t[h]).astype(BF16)
        g = 4 * lax.rem(h, 4) + lax.div(h, 4)
        at = pl.ds(pl.multiple_of(16 * g, 16), 16)
        gre[:, at, :] = got[: bands * 16].reshape(bands, 16, 256)
        gim[:, at, :] = got[bands * 16 :].reshape(bands, 16, 256)

    def local(z):
        ve, vo = pots[z, :half], pots[z, half:]
        every = range(bands)
        ys = []
        for b in every:
            re, im = gre[b], gim[b]
            a = jnp.concatenate([re[:, :128], im[:, :128]], axis=1)
            c = jnp.concatenate([re[:, 128:], im[:, 128:]], axis=1)
            ys.append((dot(a + c, yf[0][...]).astype(BF16), dot(a - c, yf[1][...]).astype(BF16)))
        xs = []
        for b in every:
            e, o = ys[b]
            re = jnp.concatenate([e[:, :128], o[:, :128]], axis=1)
            im = jnp.concatenate([e[:, 128:], o[:, 128:]], axis=1)
            a = jnp.concatenate([re[:mid], im[:mid]], axis=0)
            c = jnp.concatenate([re[mid:], im[mid:]], axis=0)
            we = (dot(xf[0][...], a + c) * jnp.concatenate([ve, ve], axis=0)).astype(BF16)
            wo = (dot(xf[1][...], a - c) * jnp.concatenate([vo, vo], axis=0)).astype(BF16)
            xs.append((we, wo))
        bs = []
        for b in every:
            e = dot(xb[0][...], xs[b][0])
            o = dot(xb[1][...], xs[b][1])
            bs.append(((e + o).astype(BF16), (e - o).astype(BF16)))
        for b in every:
            p, m = bs[b]
            re = jnp.concatenate([p[:mid], m[:mid]], axis=0)
            im = jnp.concatenate([p[mid:], m[mid:]], axis=0)
            e = dot(jnp.concatenate([re[:, :128], im[:, :128]], axis=1), yb[0][...])
            o = dot(jnp.concatenate([re[:, 128:], im[:, 128:]], axis=1), yb[1][...])
            p, m = (e + o).astype(BF16), (e - o).astype(BF16)
            back[b] = jnp.concatenate([p[:, :128], m[:, :128]], axis=1)
            back[bands + b] = jnp.concatenate([p[:, 128:], m[:, 128:]], axis=1)

    around = [lax.rem(batch + o, 4) for o in range(4)]
    across = [lax.rem(lax.div(me, 16) + o, 4) for o in range(4)]
    inside = [lax.rem(lax.rem(me, 4) + o, 4) for o in range(4)]

    def section(z, turns):
        line = lax.broadcasted_iota(jnp.int32, (16, parts * 16), 1)
        row = lax.broadcasted_iota(jnp.int32, (16, parts * 16), 0)
        ones = (lax.div(line, 16) == row).astype(F32).astype(BF16)
        spots = [(4 * around[o] + k, 4 * k + around[o]) for o in turns for k in range(4)]
        cut = []
        for h, g in spots:
            at = pl.ds(pl.multiple_of(16 * g, 16), 16)
            t = dot(back[:, at, :].reshape(parts * 16, 256), ymask[h])
            t = t.astype(BF16).reshape(parts, 16, wide) * xmask[h][None]
            cut.append(t.reshape(parts * 16, wide))
        for t, (h, g) in zip(cut, spots, strict=True):
            got = dot(ones, t)[:parts]
            for d in range(4):
                send2[z, 4 * h + d] = got[:, sticks * d : sticks * (d + 1)].astype(BF16)
        for o in turns:
            for y in (2, 1, 3, 0):
                for r in (2, 1, 3, 0):
                    spot = 16 * around[o] + 4 * across[y] + inside[r]
                    peer = 16 * across[y] + 4 * around[o] + inside[r]
                    if o or y or r:
                        start_to(send2.at[z, spot], recv2.at[z, me], bwd_s.at[z], bwd_r.at[z], "fft", peer)
                    else:
                        pltpu.make_async_copy(send2.at[z, spot], recv2.at[z, me], bwd_r.at[z]).start()

    def work(z):
        with jax.named_scope("local"):
            local(z)

        with jax.named_scope("pick"):
            section(z, (2, 3))
            section(z, (1, 0))

    def overlaps():
        wait_bytes(pall, prev_r)
        for t in range(teams):
            right = jnp.concatenate(
                [pall[t, i][p : p + 1] for p in range(2) for i in range(bands)], axis=0
            )
            part = dot_nt(left[...], right)
            part = jnp.concatenate(
                [part, jnp.zeros((2 * subs, 128 - parts), F32)], axis=1
            )
            for j in range(subs):
                r1[t, j] = part[2 * j : 2 * j + 2, :]
        for mate in mates:
            start_to(r1.at[mate], r2.at[team], one_s, one_r, "band", mate)
        pltpu.make_async_copy(r1.at[team], r2.at[team], one_r).start()

    def first(i, carry):
        q = lax.rem(batch + near(i), 4)
        wait_bytes(cols.at[pl.ds(16 * q, 16)], col_r.at[q])
        for k in range(4):
            masks(4 * q + k)
        wait_bytes(recv.at[0, pl.ds(16 * q, 16)], first_r.at[q])
        for k in range(4):
            scatter(0, 4 * q + k)
        return carry

    with jax.named_scope("first"):
        lax.fori_loop(0, 4, first, 0)

    def plane(z, carry):
        @pl.when(z > 0)
        def _():
            wait_bytes(recv.at[z], fwd_r.at[z])

            def step(h, carry):
                scatter(z, h)
                return carry

            with jax.named_scope("scatter"):
                lax.fori_loop(0, groups, step, 0, unroll=8)

        work(z)

        @pl.when(z == 0)
        def _():
            overlaps()

        return carry

    lax.fori_loop(0, depth, plane, 0)

    with jax.named_scope("inter2"):
        wait_bytes(r2, one_r)
        for peer in peers:
            start_to(
                r2.at[lax.div(peer, subs), lax.rem(peer, subs)], r3.at[me], two_s, two_r, "fft", peer
            )
        pltpu.make_async_copy(
            r2.at[lax.div(me, subs), lax.rem(me, subs)], r3.at[me], two_r).start()

    with jax.named_scope("waitback"):
        col = column[...]
        x = lax.div(col, grid)
        y = col - x * grid
        coords = jnp.concatenate([x, y, x, y, x, y, x, y], axis=0).astype(F32).astype(BF16)
        coords = jnp.concatenate([coords, coords], axis=1)
        shot[...] = low_hot[:sticks] + low_hot[sticks:]

        def unpack(z):
            wait_bytes(recv2.at[z], bwd_r.at[z])
            for f in range(owners):
                stage[z, parts * f : parts * (f + 1), :] = recv2[z, f].astype(F32)

        def column_of(z, p, b):
            return stage[z, pl.ds(p * bands + b, owners, stride=parts), :].astype(BF16)

        for z in range(depth - 1):
            unpack(z)
    with jax.named_scope("zback"):
        nothing = jnp.zeros((owners, sticks), BF16)
        lines = []
        for b in range(bands):
            field = jnp.concatenate(
                [piece for p in range(2)
                 for piece in [*[column_of(z, p, b) for z in range(depth - 1)], nothing]], axis=0
            )
            for p in range(2):
                done = dot(zb[p][...], field).astype(BF16)
                lines.append(jnp.concatenate([done[:half], done[half:]], axis=1))
        lines = jnp.concatenate(lines, axis=0)
    with jax.named_scope("pickw"):
        for c in range(0, waves, chunk):
            cut = slice(c, c + chunk)
            plane_at = lax.div(slot[:, cut], sticks)
            low_cut = low_hot[:, cut]
            xy = dot(coords, low_cut)
            fz = frequency(plane_at, grid)
            fx = frequency(xy[0:1].astype(jnp.int32), grid)
            fy = frequency(xy[1:2].astype(jnp.int32), grid)
            kinetic = (fz * fz + fx * fx + fy * fy) * (2.0 / (grid * grid))
            t = dot(lines, low_cut).reshape(parts, half, chunk)
            got = jnp.sum(t * high_hot[:, cut].astype(F32)[None], axis=1)
            for b in range(bands):
                sofar[2 * b : 2 * b + 2, cut] = (
                    got[2 * b : 2 * b + 2] + kinetic * orb[b, :, cut].astype(F32)
                )
            turns = dot(held[17][...], high_hot[:, cut])
            even = lax.rem(plane_at, 2) == 0
            for p in range(2):
                swing[p, :, cut] = jnp.where(
                    even,
                    turns[p * owners : (p + 1) * owners],
                    turns[(2 + p) * owners : (3 + p) * owners],
                )
    with jax.named_scope("last"):
        unpack(depth - 1)
        field = jnp.concatenate(
            [column_of(depth - 1, p, b) for b in range(bands) for p in range(2)], axis=0
        )
        for c in range(0, waves, chunk):
            cut = slice(c, c + chunk)
            t = dot(field, shot[:, cut])
            wr, wi = swing[0, :, cut], swing[1, :, cut]
            for b in range(bands):
                re = t[2 * b * owners : (2 * b + 1) * owners]
                im = t[(2 * b + 1) * owners : (2 * b + 2) * owners]
                got = jnp.concatenate(
                    [jnp.sum(re * wr - im * wi, axis=0, keepdims=True),
                     jnp.sum(re * wi + im * wr, axis=0, keepdims=True)], axis=0
                )
                out[b, :, cut] = (sofar[2 * b : 2 * b + 2, cut] + got).astype(BF16)

    with jax.named_scope("waits"):
        wait_bytes(r3, two_r)
        total = jnp.sum(r3[...], axis=0)
        moved = pltpu.roll(total, 128 - bands, 1)
        inter[0] = (total[0:1] + moved[1:2])[:, :bands]
        inter[1] = (moved[0:1] - total[1:2])[:, :bands]
        rest = pl.ds(0, owners - 1)
        for z in range(depth):
            wait_bytes(send.at[z, rest], fwd_s.at[z])
            wait_bytes(send2.at[z, rest], bwd_s.at[z])
        wait_bytes(cols.at[rest], col_s)
        wait_bytes(r3.at[rest], two_s)
        wait_bytes(pall.at[pl.ds(0, teams - 1)], prev_s)
        wait_bytes(r1.at[pl.ds(0, teams - 1)], one_s)


def deliver(applied, inter, out, sums, sems):
    copies = [
        pltpu.make_async_copy(applied, out, sems.at[0]),
        pltpu.make_async_copy(inter, sums, sems.at[1]),
    ]
    for copy in copies:
        copy.start()
    for copy in copies:
        copy.wait()


def per_device(orbitals, sphere_slot, stick_column, potential, subspace, previous):
    owners = lax.axis_size("fft")
    teams = lax.axis_size("band")
    groups = owners // 4
    depth, grid, _ = potential.shape
    sticks = stick_column.shape[0]
    waves = sphere_slot.shape[0]
    bands = orbitals.shape[0]
    subs = subspace.shape[0]
    parts = 2 * bands
    half = grid // 2
    every = tables(grid, owners)
    given = [
        orbitals,
        sphere_slot.reshape(1, waves),
        stick_column.reshape(1, sticks),
        potential,
        subspace,
        previous,
        *every,
    ]
    dims = (owners, groups, grid, depth, sticks, waves, bands, teams, subs)
    message = pltpu.VMEM((depth, owners, parts, sticks), BF16)
    sums = pltpu.VMEM((teams, subs, 2, 128), F32)
    one = pltpu.SemaphoreType.DMA
    four = pltpu.SemaphoreType.DMA((4,))
    several = pltpu.SemaphoreType.DMA((depth,))
    applied, inter = pl.pallas_call(
        functools.partial(kernel, dims),
        out_shape=[
            pltpu.VMEM(orbitals.shape, BF16),
            pltpu.VMEM((2, 1, bands), F32),
        ],
        in_specs=[pl.BlockSpec(memory_space=pl.ANY) for _ in range(6 + len(every))],
        out_specs=[vmem(), vmem()],
        scratch_shapes=[
            *[pltpu.VMEM(t.shape, t.dtype) for t in given if t is not previous],
            pltpu.VMEM((depth, owners * parts, sticks), F32),
            message,
            message,
            message,
            message,
            pltpu.VMEM((owners, 1, sticks), jnp.int32),
            pltpu.VMEM((groups, parts, 4 * sticks), F32),
            pltpu.VMEM((depth, grid, 256), F32),
            pltpu.VMEM((2, grid, 128), F32),
            pltpu.VMEM((teams, *previous.shape), BF16),
            sums,
            sums,
            pltpu.VMEM((owners, 2, 128), F32),
            pltpu.VMEM((parts, waves), F32),
            pltpu.VMEM((2, owners, waves), F32),
            pltpu.SemaphoreType.DMA((18,)),
            one, four, several, four, several, several, several, one, one, one, one, one, one,
        ],
        compiler_params=pltpu.CompilerParams(
            vmem_limit_bytes=60 * 2**20, collective_id=0, has_side_effects=True
        ),
        name="apply",
    )(*given)
    return tuple(pl.pallas_call(
        deliver,
        out_shape=[
            jax.ShapeDtypeStruct(orbitals.shape, BF16),
            jax.ShapeDtypeStruct((2, 1, bands), F32),
        ],
        in_specs=[vmem(), vmem()],
        out_specs=[pl.BlockSpec(memory_space=pl.ANY)] * 2,
        scratch_shapes=[pltpu.SemaphoreType.DMA((2,))],
        name="deliver",
    )(pltpu.with_memory_space_constraint(applied, pltpu.VMEM), pltpu.with_memory_space_constraint(inter, pltpu.VMEM)))


def solution(mesh):
    return jax.shard_map(
        per_device,
        mesh=mesh,
        in_specs=(
            P("band", None, "fft"),
            P("fft"),
            P("fft"),
            P("fft", None, None),
            P("band", None, "fft"),
            P("band", None, "fft"),
        ),
        out_specs=(P("band", None, "fft"), P(None, "fft", "band")),
        check_vma=False,
    )
```
